128 devices in a mesh: fsdp: 128 (over z, y, x, core).
Axes of the slice: x: 4, y: 4, z: 4, core: 2. Of those that a mesh axis runs over, the one named last changes fastest.
Arguments:
- tok_ids: int32 [524288], P('fsdp')
- tok_labels: int32 [524288], P('fsdp')
- loss_mask: int32 [524288], P('fsdp')
- emb_table: bfloat16 [2048, 256], P('fsdp')
- gain_mlp: float32 [256], replicated
- gain_head: float32 [256], replicated
- w_gate: bfloat16 [256, 768], P('fsdp')
- w_up: bfloat16 [256, 768], P('fsdp')
- w_down: bfloat16 [768, 256], P('fsdp')
Outputs:
- output 1: float32 [], replicated
- output 2: float32 [2048, 256], P('fsdp')
- output 3: float32 [256, 768], P('fsdp')
- output 4: float32 [256, 768], P('fsdp')
- output 5: float32 [768, 256], P('fsdp')
All inputs are finite; a program needn't handle non-finite values.
Results may differ from the reference program's by a relative error of at most 0.00844.
Values are sent between devices in bfloat16 or wider.
A program may use at most 1 GiB of HBM per device.

```python
import jax
import jax.numpy as jnp
from jax import lax

VOCAB = 2048
D_MODEL = 256
D_FF = 768
TOK_DEV = 4096
GROUP_SIZE = 128
T_GLOBAL = TOK_DEV * GROUP_SIZE
NORM_EPS = 1e-6
ROW_CONTRACT = (((1,), (1,)), ((), ()))
TOK_CONTRACT = (((0,), (0,)), ((), ()))


def draw_tokens(tok_key):
    key_ids, key_lab, key_pad, key_cut = jax.random.split(tok_key, 4)
    tok_ids = jax.random.randint(key_ids, (T_GLOBAL,), 0, VOCAB, dtype=jnp.int32)
    tok_ids = tok_ids.at[0].set(0).at[1].set(VOCAB - 1)
    tok_labels = jax.random.randint(key_lab, (T_GLOBAL,), 0, VOCAB, dtype=jnp.int32)
    tok_labels = tok_labels.at[0].set(VOCAB - 1).at[1].set(0)
    pad_len = jax.random.randint(key_pad, (GROUP_SIZE, 1), 0, TOK_DEV // 2 + 1, dtype=jnp.int32)
    keep_tail = jnp.arange(TOK_DEV)[None, :] < TOK_DEV - pad_len
    cut_draw = jax.random.randint(key_cut, (GROUP_SIZE, TOK_DEV), 0, 16, dtype=jnp.int32)
    loss_mask = (keep_tail & (cut_draw != 0)).astype(jnp.int32).reshape(T_GLOBAL)
    return tok_ids, tok_labels, loss_mask.at[0].set(1)


def setup_inputs(seed: int = 0) -> dict:
    root_key = jax.random.key(seed)
    key_tok, key_emb, key_g1, key_g2, key_gate, key_up, key_down = jax.random.split(root_key, 7)
    tok_ids, tok_labels, loss_mask = draw_tokens(key_tok)
    emb_table = (jax.random.normal(key_emb, (VOCAB, D_MODEL), jnp.float32) * D_MODEL ** -0.5).astype(jnp.bfloat16)
    gain_mlp = 1.0 + 0.5 * jax.random.normal(key_g1, (D_MODEL,), jnp.float32)
    gain_head = 1.0 + 0.5 * jax.random.normal(key_g2, (D_MODEL,), jnp.float32)
    w_gate = (jax.random.normal(key_gate, (D_MODEL, D_FF), jnp.float32) * D_MODEL ** -0.5).astype(jnp.bfloat16)
    w_up = (jax.random.normal(key_up, (D_MODEL, D_FF), jnp.float32) * D_MODEL ** -0.5).astype(jnp.bfloat16)
    w_down = (jax.random.normal(key_down, (D_FF, D_MODEL), jnp.float32) * 1.5 * (D_FF * D_MODEL) ** -0.5).astype(jnp.bfloat16)
    return {"tok_ids": tok_ids, "tok_labels": tok_labels, "loss_mask": loss_mask, "emb_table": emb_table, "gain_mlp": gain_mlp, "gain_head": gain_head, "w_gate": w_gate, "w_up": w_up, "w_down": w_down}


def rms_scale(rows_wide, norm_gain):
    inv_rms = lax.rsqrt(jnp.mean(rows_wide * rows_wide, axis=-1, keepdims=True) + NORM_EPS)
    return (rows_wide * inv_rms * norm_gain).astype(jnp.bfloat16), inv_rms


def rms_back(rows_wide, inv_rms, norm_gain, grad_out):
    scaled_grad = grad_out * norm_gain
    return inv_rms * (scaled_grad - rows_wide * (inv_rms * inv_rms) * jnp.mean(scaled_grad * rows_wide, axis=-1, keepdims=True))


def mlp_forward(emb_rows, gain_mlp, gain_head, w_gate, w_up, w_down):
    emb_wide = emb_rows.astype(jnp.float32)
    a_norm, inv_first = rms_scale(emb_wide, gain_mlp)
    gate_wide = jnp.dot(a_norm, w_gate, preferred_element_type=jnp.float32).astype(jnp.bfloat16).astype(jnp.float32)
    up_wide = jnp.dot(a_norm, w_up, preferred_element_type=jnp.float32).astype(jnp.bfloat16).astype(jnp.float32)
    gate_sig = jax.nn.sigmoid(gate_wide)
    act_rows = (gate_wide * gate_sig * up_wide).astype(jnp.bfloat16)
    hid_wide = (emb_wide + jnp.dot(act_rows, w_down, preferred_element_type=jnp.float32)).astype(jnp.bfloat16).astype(jnp.float32)
    h_norm, inv_second = rms_scale(hid_wide, gain_head)
    return (emb_wide, inv_first, a_norm, gate_wide, up_wide, gate_sig, act_rows, hid_wide, inv_second), h_norm


def head_forward(h_norm, emb_table, tok_labels, tok_coef):
    logits = lax.dot_general(h_norm, emb_table, ROW_CONTRACT, preferred_element_type=jnp.float32)
    row_max = jnp.max(logits, axis=-1, keepdims=True)
    exp_rows = jnp.exp(logits - row_max)
    sum_exp = jnp.sum(exp_rows, axis=-1, keepdims=True)
    is_label = jnp.arange(logits.shape[1])[None, :] == tok_labels[:, None]
    picked = jnp.sum(jnp.where(is_label, logits, 0.0), axis=-1)
    tok_loss = row_max[:, 0] + jnp.log(sum_exp[:, 0]) - picked
    d_logits = ((exp_rows / sum_exp - is_label.astype(jnp.float32)) * tok_coef[:, None]).astype(jnp.bfloat16)
    return jnp.sum(tok_coef * tok_loss), d_logits


def mlp_backward(saved, d_hidden, gain_mlp, w_gate, w_up, w_down):
    emb_wide, inv_first, a_norm, gate_wide, up_wide, gate_sig, act_rows = saved[:7]
    hid_grad = d_hidden.astype(jnp.bfloat16)
    d_act = lax.dot_general(hid_grad, w_down, ROW_CONTRACT, preferred_element_type=jnp.float32)
    grad_down = lax.dot_general(act_rows, hid_grad, TOK_CONTRACT, preferred_element_type=jnp.float32)
    d_up = (d_act * gate_wide * gate_sig).astype(jnp.bfloat16)
    d_gate = (d_act * up_wide * gate_sig * (1.0 + gate_wide * (1.0 - gate_sig))).astype(jnp.bfloat16)
    grad_gate = lax.dot_general(a_norm, d_gate, TOK_CONTRACT, preferred_element_type=jnp.float32)
    grad_up = lax.dot_general(a_norm, d_up, TOK_CONTRACT, preferred_element_type=jnp.float32)
    d_anorm = lax.dot_general(d_gate, w_gate, ROW_CONTRACT, preferred_element_type=jnp.float32) + lax.dot_general(d_up, w_up, ROW_CONTRACT, preferred_element_type=jnp.float32)
    grad_x = d_hidden + rms_back(emb_wide, inv_first, gain_mlp, d_anorm)
    return grad_x, grad_gate, grad_up, grad_down


def block_grads(tok_ids, tok_labels, tok_coef, emb_table, gain_mlp, gain_head, w_gate, w_up, w_down):
    saved, h_norm = mlp_forward(jnp.take(emb_table, tok_ids, axis=0), gain_mlp, gain_head, w_gate, w_up, w_down)
    loss_part, d_logits = head_forward(h_norm, emb_table, tok_labels, tok_coef)
    d_hnorm = jnp.dot(d_logits, emb_table, preferred_element_type=jnp.float32)
    head_grad = lax.dot_general(d_logits, h_norm, TOK_CONTRACT, preferred_element_type=jnp.float32)
    d_hidden = rms_back(saved[7], saved[8], gain_head, d_hnorm)
    grad_x, grad_gate, grad_up, grad_down = mlp_backward(saved, d_hidden, gain_mlp, w_gate, w_up, w_down)
    grad_table = head_grad + jax.ops.segment_sum(grad_x, tok_ids, num_segments=emb_table.shape[0])
    return loss_part, grad_table, grad_gate, grad_up, grad_down


def reference(tok_ids, tok_labels, loss_mask, emb_table, gain_mlp, gain_head, w_gate, w_up, w_down):
    mask_wide = loss_mask.astype(jnp.float32)
    tok_coef = (mask_wide / jnp.sum(mask_wide)).reshape(GROUP_SIZE, TOK_DEV)

    def scan_step(acc_state, block_in):
        step_out = block_grads(block_in[0], block_in[1], block_in[2], emb_table, gain_mlp, gain_head, w_gate, w_up, w_down)
        return tuple(prev_val + new_val for prev_val, new_val in zip(acc_state, step_out)), None

    init_state = (jnp.zeros((), jnp.float32), jnp.zeros((VOCAB, D_MODEL), jnp.float32), jnp.zeros((D_MODEL, D_FF), jnp.float32), jnp.zeros((D_MODEL, D_FF), jnp.float32), jnp.zeros((D_FF, D_MODEL), jnp.float32))
    blocks = (tok_ids.reshape(GROUP_SIZE, TOK_DEV), tok_labels.reshape(GROUP_SIZE, TOK_DEV), tok_coef)
    final_state, _ = lax.scan(scan_step, init_state, blocks)
    loss_val, grad_table, grad_gate, grad_up, grad_down = final_state
    return (loss_val, grad_table, grad_gate, grad_up, grad_down)
```

```python
import functools

import jax
import jax.numpy as jnp
from jax import lax
from jax.experimental import pallas as pl
from jax.experimental.pallas import tpu as pltpu
from jax.sharding import PartitionSpec as P

NORM_EPS = 1e-6
ROW_CONTRACT = (((1,), (1,)), ((), ()))
MESH = pl.DeviceIdType.MESH
AXIS = "fsdp"
STRIDES = (2, 8, 32)
N_STREAM = 6
AG_ROWS = 96
AG_GATE, AG_UP, AG_DOWN, AG_CNT = 32, 44, 56, 68
RS_ROWS = 72
RS_GATE, RS_UP, RS_DOWN, RS_LOSS = 32, 44, 56, 68
RS_STREAMS = ((0, 16), (16, 16), (32, 16), (48, 8), (56, 8), (64, 8))


def torus_partner(v, t):
    near = v + 1 - 2 * lax.rem(v, 2)
    far = 3 - v
    return near + t * (far - near)


def my_place():
    me = lax.axis_index(AXIS)
    core = lax.rem(me, 2)
    coords = (lax.rem(lax.div(me, 2), 4), lax.rem(lax.div(me, 8), 4), lax.div(me, 32))
    return me, core, coords


def greet(me, core, coords):
    barrier = pltpu.get_barrier_semaphore()
    pl.semaphore_signal(barrier, inc=1, device_id=(me + 1 - 2 * core,), device_id_type=MESH)
    for d in range(3):
        for t in range(2):
            other = me + (torus_partner(coords[d], t) - coords[d]) * STRIDES[d]
            pl.semaphore_signal(barrier, inc=1, device_id=(other,), device_id_type=MESH)
    return barrier


def link_of(k, s, core):
    return (k + s) % 3, lax.rem(core + ((k + s) // 3) % 2, 2)


def send_copy(src, dst, send_sem, recv_sem, target):
    return pltpu.make_async_remote_copy(src_ref=src, dst_ref=dst, send_sem=send_sem, recv_sem=recv_sem, device_id=(target,), device_id_type=MESH)


def gather_kernel(e_ref, wg_ref, wu_ref, wd_ref, mask_ref, out_ref, buf, pack, send_sem, recv_sem, side_send, side_recv, out_sem):
    me, core, coords = my_place()
    cx, cy, cz = coords
    barrier = greet(me, core, coords)
    wide = jnp.float32
    pack[0:16, :] = e_ref[:, 0:128].astype(wide)
    pack[16:32, :] = e_ref[:, 128:256].astype(wide)
    for base, ref in ((AG_GATE, wg_ref), (AG_UP, wu_ref), (AG_DOWN, wd_ref)):
        vals = ref[...].astype(wide)
        tiles = vals.shape[1] // 128
        for r in range(vals.shape[0]):
            for c in range(tiles):
                row = base + r * tiles + c
                pack[row:row + 1, :] = vals[r:r + 1, c * 128:(c + 1) * 128]
    pack[AG_CNT:AG_ROWS, :] = jnp.zeros((AG_ROWS - AG_CNT, 128), wide)
    pack[AG_CNT:AG_CNT + 1, :] = jnp.sum(mask_ref[...].astype(wide), axis=0, keepdims=True)
    buf[cz, cy, cx, core] = pack[...].astype(jnp.bfloat16)
    pl.semaphore_wait(barrier, 7)

    def pieces(k, s):
        held = []
        for d in range(3):
            done = [q for q in range(s) if (k + q) % 3 == d]
            v = coords[d]
            if not done:
                held.append([pl.ds(v, 1)])
            elif len(done) == 1:
                _, t = link_of(k, done[0], core)
                held.append([pl.ds(v, 1), pl.ds(torus_partner(v, t), 1)])
            else:
                held.append([pl.ds(0, 4)])
        return [(iz, iy, ix) for iz in held[2] for iy in held[1] for ix in held[0]]

    pending = {}
    for s in range(6):
        for k in range(N_STREAM):
            if s > 0:
                for c in pending[k, s - 1]:
                    c.wait_recv()
            d, t = link_of(k, s, core)
            target = me + (torus_partner(coords[d], t) - coords[d]) * STRIDES[d]
            base = sum(len(pending[k, q]) for q in range(s))
            copies = []
            for i, (iz, iy, ix) in enumerate(pieces(k, s)):
                ref = buf.at[iz, iy, ix, core, pl.ds(16 * k, 16), :]
                c = send_copy(ref, ref, send_sem.at[k, base + i], recv_sem.at[k, base + i], target)
                c.start()
                copies.append(c)
            pending[k, s] = copies
    last = []
    for k in range(N_STREAM):
        for c in pending[k, 5]:
            c.wait_recv()
        ref = buf.at[:, :, :, core, pl.ds(16 * k, 16), :]
        c = send_copy(ref, ref, side_send.at[k], side_recv.at[k], me + 1 - 2 * core)
        c.start()
        last.append(c)
    for c in last:
        c.wait_recv()
    out = pltpu.make_async_copy(buf, out_ref, out_sem)
    out.start()
    for copies in pending.values():
        for c in copies:
            c.wait_send()
    for c in last:
        c.wait_send()
    out.wait()


def gather_all(table_shard, gate_shard, up_shard, down_shard, mask):
    vm = pl.BlockSpec(memory_space=pltpu.VMEM)
    return pl.pallas_call(
        gather_kernel,
        out_shape=jax.ShapeDtypeStruct((4, 4, 4, 2, AG_ROWS, 128), jnp.bfloat16),
        in_specs=[vm] * 5,
        out_specs=pl.BlockSpec(memory_space=pl.ANY),
        scratch_shapes=[
            pltpu.VMEM((4, 4, 4, 2, AG_ROWS, 128), jnp.bfloat16),
            pltpu.VMEM((AG_ROWS, 128), jnp.float32),
            pltpu.SemaphoreType.DMA((N_STREAM, 21)),
            pltpu.SemaphoreType.DMA((N_STREAM, 21)),
            pltpu.SemaphoreType.DMA((N_STREAM,)),
            pltpu.SemaphoreType.DMA((N_STREAM,)),
            pltpu.SemaphoreType.DMA,
        ],
        compiler_params=pltpu.CompilerParams(collective_id=0, has_side_effects=True, vmem_limit_bytes=32 << 20),
        name="gather_all",
    )(table_shard, gate_shard, up_shard, down_shard, mask)


def recv_shape(k, s):
    sizes = [4, 4, 4]
    for q in range(s + 1):
        sizes[(k + q) % 3] //= 2
    return sizes[2], sizes[1], sizes[0]


def reduce_kernel(g_ref, *refs):
    loss_ref, e_out, wg_out, wu_out, wd_out = refs[:5]
    acc, side, res = refs[5:8]
    recv = refs[8:8 + 36]
    send_sem, recv_sem, side_send, side_recv, own_sem = refs[44:]
    me, core, coords = my_place()
    barrier = greet(me, core, coords)
    own = []
    for k, (r0, rn) in enumerate(RS_STREAMS):
        c = pltpu.make_async_copy(g_ref.at[:, :, :, core, pl.ds(r0, rn), :], acc.at[:, :, :, pl.ds(r0, rn), :], own_sem.at[k])
        c.start()
        own.append(c)
    pl.semaphore_wait(barrier, 7)
    sides = []
    for k, (r0, rn) in enumerate(RS_STREAMS):
        c = send_copy(g_ref.at[:, :, :, 1 - core, pl.ds(r0, rn), :], side.at[:, :, :, pl.ds(r0, rn), :], side_send.at[k], side_recv.at[k], me + 1 - 2 * core)
        c.start()
        sides.append(c)

    def at_dim(d, idx):
        full = [slice(None)] * 3
        full[2 - d] = idx
        return tuple(full)

    pending = {}
    for s in range(7):
        for k, (r0, rn) in enumerate(RS_STREAMS):
            rows = pl.ds(r0, rn)
            if s == 0:
                own[k].wait()
                sides[k].wait_recv()
                acc[:, :, :, rows, :] += side[:, :, :, rows, :]
                cur = acc.at[:, :, :, rows, :]
            else:
                q = s - 1
                for c in pending[k, q]:
                    c.wait_recv()
                d, t = link_of(k, q, core)
                v = coords[d]
                prev = acc.at[:, :, :, rows, :] if q == 0 else recv[k * 6 + q - 1]
                cur = recv[k * 6 + q]
                if q < 3:
                    mate = torus_partner(v, 1 - t)
                    lo = jnp.minimum(v, mate)
                    hi = jnp.maximum(v, mate)
                    for j, idx in enumerate((lo, hi)):
                        at = at_dim(d, pl.ds(j, 1))
                        cur[at] += prev[at_dim(d, pl.ds(idx, 1))]
                else:
                    mate = torus_partner(v, t)
                    keep = jnp.where(v > mate, 1, 0)
                    cur[...] += prev[at_dim(d, pl.ds(keep, 1))]
            if s == 6:
                res[rows, :] = cur[0, 0, 0]
                continue
            d, t = link_of(k, s, core)
            v = coords[d]
            mate = torus_partner(v, t)
            target = me + (mate - v) * STRIDES[d]
            dst = recv[k * 6 + s]
            copies = []
            if s < 3:
                far = torus_partner(mate, 1 - t)
                lo = jnp.minimum(mate, far)
                hi = jnp.maximum(mate, far)
                for j, idx in enumerate((lo, hi)):
                    c = send_copy(cur.at[at_dim(d, pl.ds(idx, 1))], dst.at[at_dim(d, pl.ds(j, 1))], send_sem.at[k, 2 * s + j], recv_sem.at[k, 2 * s + j], target)
                    c.start()
                    copies.append(c)
            else:
                give = jnp.where(v > mate, 0, 1)
                c = send_copy(cur.at[at_dim(d, pl.ds(give, 1))], dst, send_sem.at[k, 3 + s], recv_sem.at[k, 3 + s], target)
                c.start()
                copies.append(c)
            pending[k, s] = copies
    loss_ref[...] = res[RS_LOSS:RS_LOSS + 1, :]
    e_out[:, 0:128] = res[0:16, :]
    e_out[:, 128:256] = res[16:32, :]
    for base, ref in ((RS_GATE, wg_out), (RS_UP, wu_out), (RS_DOWN, wd_out)):
        tiles = ref.shape[1] // 128
        for r in range(ref.shape[0]):
            for c in range(tiles):
                row = base + r * tiles + c
                ref[r:r + 1, c * 128:(c + 1) * 128] = res[row:row + 1, :]
    for copies in pending.values():
        for c in copies:
            c.wait_send()
    for c in sides:
        c.wait_send()


def reduce_all(grads):
    vm = pl.BlockSpec(memory_space=pltpu.VMEM)
    sds = lambda *shape: jax.ShapeDtypeStruct(shape, jnp.float32)
    recvs = [pltpu.VMEM((*recv_shape(k, s), rn, 128), jnp.float32) for k, (_, rn) in enumerate(RS_STREAMS) for s in range(6)]
    return pl.pallas_call(
        reduce_kernel,
        out_shape=(sds(1, 128), sds(16, 256), sds(2, 768), sds(2, 768), sds(6, 256)),
        in_specs=[pl.BlockSpec(memory_space=pl.ANY)],
        out_specs=(vm,) * 5,
        scratch_shapes=[
            pltpu.VMEM((4, 4, 4, RS_ROWS, 128), jnp.float32),
            pltpu.VMEM((4, 4, 4, RS_ROWS, 128), jnp.float32),
            pltpu.VMEM((RS_ROWS, 128), jnp.float32),
            *recvs,
            pltpu.SemaphoreType.DMA((N_STREAM, 9)),
            pltpu.SemaphoreType.DMA((N_STREAM, 9)),
            pltpu.SemaphoreType.DMA((N_STREAM,)),
            pltpu.SemaphoreType.DMA((N_STREAM,)),
            pltpu.SemaphoreType.DMA((N_STREAM,)),
        ],
        compiler_params=pltpu.CompilerParams(collective_id=1, has_side_effects=True, vmem_limit_bytes=32 << 20),
        name="reduce_all",
    )(grads)


TILE = 512
N_TILE = 4096 // TILE
V_CHUNK = 512
F_CHUNK = 256


def mm(a, b):
    return jnp.dot(a, b, preferred_element_type=jnp.float32)


def mm_nt(a, b):
    return lax.dot_general(a, b, ROW_CONTRACT, preferred_element_type=jnp.float32)


def step_kernel(gath, ids, labels, mask, g1, g2, g_out, loss_out, e_s, et_s, wg_s, wgt_s, wu_s, wut_s, wd_s, wdt_s, g1_s, g2_s, d_e, d_wg, d_wu, d_wd, logit_s, dl_s, oh_s, sl_s, dp_s, u_s, dh_s, dq_s, dpb_s, stage):
    f32, bf16 = jnp.float32, jnp.bfloat16
    rows = g_out.reshape(128 * RS_ROWS, 128)
    g_out[:, 0:48, :] = gath[:, 32:80, :].astype(f32)
    for base, acc, w, wt in ((AG_GATE, d_wg, wg_s, wgt_s), (AG_UP, d_wu, wu_s, wut_s), (AG_DOWN, d_wd, wd_s, wdt_s)):
        n = acc.shape[0]
        per, tiles = n // 128, acc.shape[1] // 128
        for c in range(tiles):
            for r in range(per):
                stage[pl.ds(c * n + r, 128, stride=per), :] = rows[pl.ds(base - 32 + r * tiles + c, 128, stride=RS_ROWS), :]
            acc[:, c * 128:(c + 1) * 128] = stage[c * n:(c + 1) * n, :]
        w[...] = acc[...].astype(bf16)
        wt[...] = acc[...].T.astype(bf16)
        acc[...] = jnp.zeros_like(acc)
    total = jnp.sum(g_out[:, AG_CNT - 32, :])
    for half in range(2):
        part = gath[:, 16 * half:16 * half + 16, :].reshape(2048, 128)
        e_s[:, 128 * half:128 * half + 128] = part
        et_s[128 * half:128 * half + 128, :] = part.T
    g1_s[...] = jnp.broadcast_to(g1[...], (128, 256)).T
    g2_s[...] = jnp.broadcast_to(g2[...], (128, 256)).T
    d_e[...] = jnp.zeros_like(d_e)
    loss_out[...] = jnp.zeros_like(loss_out)

    def wide_gain(ref):
        return jnp.concatenate([ref[...]] * (TILE // 128), axis=1)

    def norm(x, gain):
        r = lax.rsqrt(jnp.mean(x * x, axis=0, keepdims=True) + NORM_EPS)
        return (x * r * gain).astype(bf16), r

    def norm_back(x, r, gain, grad):
        sg = grad * gain
        return r * (sg - x * (r * r) * jnp.mean(sg * x, axis=0, keepdims=True))

    def tile_step(i, carry):
        id_row, label_row = ids[i], labels[i]
        coef = mask[i].astype(f32) / total
        for v in range(0, 2048, V_CHUNK):
            vocab = lax.broadcasted_iota(jnp.int32, (V_CHUNK, TILE), 0) + v
            oh_s[v:v + V_CHUNK, :] = jnp.where(vocab == id_row, 1.0, 0.0).astype(bf16)
        x = mm(et_s[...], oh_s[...])
        gain1, gain2 = wide_gain(g1_s), wide_gain(g2_s)
        a, r1 = norm(x, gain1)
        for f in range(0, 768, F_CHUNK):
            sl = slice(f, f + F_CHUNK)
            p = mm(wgt_s[sl, :], a).astype(bf16).astype(f32)
            q = mm(wut_s[sl, :], a).astype(bf16).astype(f32)
            s = jax.nn.sigmoid(p)
            silu = p * s
            sl_s[sl, :] = silu
            u_s[sl, :] = (silu * q).astype(bf16)
            dp_s[sl, :] = q * s * (1.0 + p * (1.0 - s))
        h = (x + mm(wdt_s[...], u_s[...])).astype(bf16).astype(f32)
        hn, r2 = norm(h, gain2)
        top = jnp.full((1, TILE), -jnp.inf, f32)
        for v in range(0, 2048, V_CHUNK):
            part = mm(e_s[v:v + V_CHUNK, :], hn)
            logit_s[v:v + V_CHUNK, :] = part
            top = jnp.maximum(top, jnp.max(part, axis=0, keepdims=True))
        den = jnp.zeros((1, TILE), f32)
        picked = jnp.zeros((1, TILE), f32)
        for v in range(0, 2048, V_CHUNK):
            part = logit_s[v:v + V_CHUNK, :]
            vocab = lax.broadcasted_iota(jnp.int32, (V_CHUNK, TILE), 0) + v
            picked += jnp.sum(jnp.where(vocab == label_row, part, 0.0), axis=0, keepdims=True)
            part = jnp.exp(part - top)
            den += jnp.sum(part, axis=0, keepdims=True)
            logit_s[v:v + V_CHUNK, :] = part
        loss_out[...] += coef * (top + jnp.log(den) - picked)
        scale = coef / den
        for v in range(0, 2048, V_CHUNK):
            vocab = lax.broadcasted_iota(jnp.int32, (V_CHUNK, TILE), 0) + v
            part = logit_s[v:v + V_CHUNK, :] * scale
            dl_s[v:v + V_CHUNK, :] = (part - jnp.where(vocab == label_row, coef, 0.0)).astype(bf16)
        dhn = mm(et_s[...], dl_s[...])
        dh = norm_back(h, r2, gain2, dhn)
        dhb = dh.astype(bf16)
        dh_s[...] = dh
        for f in range(0, 768, F_CHUNK):
            sl = slice(f, f + F_CHUNK)
            du = mm(wd_s[sl, :], dhb)
            dq_s[sl, :] = (du * sl_s[sl, :]).astype(bf16)
            dpb_s[sl, :] = (du * dp_s[sl, :]).astype(bf16)
            d_wd[sl, :] += mm_nt(u_s[sl, :], dhb)
        d_wg[...] += mm_nt(a, dpb_s[...])
        d_wu[...] += mm_nt(a, dq_s[...])
        da = mm(wg_s[...], dpb_s[...]) + mm(wu_s[...], dq_s[...])
        dx = dh_s[...] + norm_back(x, r1, gain1, da)
        hi = dx.astype(bf16)
        rest = dx - hi.astype(f32)
        mid = rest.astype(bf16)
        low = (rest - mid.astype(f32)).astype(bf16)
        for v in range(0, 2048, V_CHUNK):
            sl = slice(v, v + V_CHUNK)
            oh = oh_s[sl, :]
            d_e[sl, :] += mm_nt(dl_s[sl, :], hn) + mm_nt(oh, hi) + mm_nt(oh, mid) + mm_nt(oh, low)
        return carry

    lax.fori_loop(0, N_TILE, tile_step, 0)

    for half in range(2):
        g_out[:, 16 * half:16 * half + 16, :] = d_e[:, 128 * half:128 * half + 128].reshape(128, 16, 128)
    for base, acc in ((RS_GATE, d_wg), (RS_UP, d_wu), (RS_DOWN, d_wd)):
        n = acc.shape[0]
        per, tiles = n // 128, acc.shape[1] // 128
        for c in range(tiles):
            stage[c * n:(c + 1) * n, :] = acc[:, c * 128:(c + 1) * 128]
            for r in range(per):
                rows[pl.ds(base + r * tiles + c, 128, stride=RS_ROWS), :] = stage[pl.ds(c * n + r, 128, stride=per), :]
    loss = jnp.sum(loss_out[...])
    for r in range(RS_LOSS, RS_ROWS):
        rows[pl.ds(r, 128, stride=RS_ROWS), :] = jnp.full((128, 128), loss, f32)


def local_step(gathered, tok_ids, tok_labels, mask, gain_mlp, gain_head):
    vm = pl.BlockSpec(memory_space=pltpu.VMEM)
    v = lambda dt, *shape: pltpu.VMEM(shape, dt)
    f32, bf16 = jnp.float32, jnp.bfloat16
    tok = lambda t: t.reshape(N_TILE, 1, TILE)
    return pl.pallas_call(
        step_kernel,
        out_shape=(jax.ShapeDtypeStruct((128, RS_ROWS, 128), f32), jax.ShapeDtypeStruct((1, TILE), f32)),
        in_specs=[vm] * 6,
        out_specs=(vm, vm),
        scratch_shapes=[
            v(bf16, 2048, 256), v(bf16, 256, 2048),
            v(bf16, 256, 768), v(bf16, 768, 256), v(bf16, 256, 768), v(bf16, 768, 256), v(bf16, 768, 256), v(bf16, 256, 768),
            v(f32, 256, 128), v(f32, 256, 128),
            v(f32, 2048, 256), v(f32, 256, 768), v(f32, 256, 768), v(f32, 768, 256),
            v(f32, 2048, TILE), v(bf16, 2048, TILE), v(bf16, 2048, TILE),
            v(f32, 768, TILE), v(f32, 768, TILE), v(bf16, 768, TILE), v(f32, 256, TILE), v(bf16, 768, TILE), v(bf16, 768, TILE), v(f32, 1536, 128),
        ],
        compiler_params=pltpu.CompilerParams(vmem_limit_bytes=62 << 20),
        name="local_step",
    )(gathered.reshape(128, AG_ROWS, 128), tok(tok_ids), tok(tok_labels), tok(mask), gain_mlp.reshape(1, 256), gain_head.reshape(1, 256))[0]


def solution(mesh):
    def device_step(tok_ids, tok_labels, loss_mask, table_shard, gain_mlp, gain_head, gate_shard, up_shard, down_shard):
        gathered = gather_all(table_shard, gate_shard, up_shard, down_shard, loss_mask.reshape(32, 128))
        grads = local_step(gathered, tok_ids, tok_labels, loss_mask, gain_mlp, gain_head)
        loss, e_out, wg_out, wu_out, wd_out = reduce_all(grads.reshape(4, 4, 4, 2, RS_ROWS, 128))
        return loss[0, 0], e_out, wg_out, wu_out, wd_out

    row_spec = P("fsdp", None)
    tok_spec = P("fsdp")
    return jax.shard_map(device_step, mesh=mesh, in_specs=(tok_spec, tok_spec, tok_spec, row_spec, P(), P(), row_spec, row_spec, row_spec), out_specs=(P(), row_spec, row_spec, row_spec, row_spec), check_vma=False)
```

```python
import functools

import jax
import jax.numpy as jnp
from jax import lax
from jax.experimental import pallas as pl
from jax.experimental.pallas import tpu as pltpu
from jax.sharding import PartitionSpec as P

NORM_EPS = 1e-6
ROW_CONTRACT = (((1,), (1,)), ((), ()))
MESH = pl.DeviceIdType.MESH
AXIS = "fsdp"
STRIDES = (2, 8, 32)
N_STREAM = 6
AG_ROWS = 96
RS_ROWS = 72
RS_GATE, RS_UP, RS_DOWN, RS_LOSS = 32, 44, 56, 68
RS_STREAMS = ((0, 16), (16, 16), (32, 16), (48, 8), (56, 8), (64, 8))


TILE = 1024
N_TILE = 4096 // TILE
V_CHUNK = 256
F_CHUNK = 256


def torus_partner(v, t):
    near = v + 1 - 2 * lax.rem(v, 2)
    far = 3 - v
    return near + t * (far - near)


def my_place():
    me = lax.axis_index(AXIS)
    core = lax.rem(me, 2)
    coords = (lax.rem(lax.div(me, 2), 4), lax.rem(lax.div(me, 8), 4), lax.div(me, 32))
    return me, core, coords


def greet(me, core, coords):
    barrier = pltpu.get_barrier_semaphore()
    pl.semaphore_signal(barrier, inc=1, device_id=(me + 1 - 2 * core,), device_id_type=MESH)
    for d in range(3):
        for t in range(2):
            other = me + (torus_partner(coords[d], t) - coords[d]) * STRIDES[d]
            pl.semaphore_signal(barrier, inc=1, device_id=(other,), device_id_type=MESH)
    return barrier


def link_of(k, s, core):
    return (k + s) % 3, lax.rem(core + ((k + s) // 3) % 2, 2)


def send_copy(src, dst, send_sem, recv_sem, target):
    return pltpu.make_async_remote_copy(src_ref=src, dst_ref=dst, send_sem=send_sem, recv_sem=recv_sem, device_id=(target,), device_id_type=MESH)


def torus_order(v, t):
    return v + t * (min_int(v, 1) * (lax.rem(v, 3) + 1) - v)


def min_int(a, b):
    return jnp.minimum(a, b)


def first_pairing(k, d, core):
    s = (d - k) % 3
    return link_of(k, s, core)[1]


def gather_send(buf, k, s, me, core, coords, send_sem, recv_sem):
    idx = []
    for d in (2, 1, 0):
        done = len([q for q in range(s) if (k + q) % 3 == d])
        p = torus_order(coords[d], first_pairing(k, d, core))
        idx.append((pl.ds(p, 1), pl.ds(2 * lax.div(p, 2), 2), pl.ds(0, 4))[done])
    d, t = link_of(k, s, core)
    target = me + (torus_partner(coords[d], t) - coords[d]) * STRIDES[d]
    ref = buf.at[(core, k, *idx)]
    return send_copy(ref, ref, send_sem.at[k, s], recv_sem.at[k, s], target)


def gather_phase(me, core, coords, barrier, shards, mask, buf, pack, send_sem, recv_sem, side_send, side_recv):
    cx, cy, cz = coords
    wide = jnp.float32
    e_ref, *w_refs = shards
    pack[0:16, :] = e_ref[:, 0:128].astype(wide)
    pack[16:32, :] = e_ref[:, 128:256].astype(wide)
    pack[32:AG_ROWS, :] = jnp.zeros((AG_ROWS - 32, 128), wide)
    for k, ref in enumerate(w_refs):
        vals = ref[...].astype(wide)
        tiles = vals.shape[1] // 128
        for r in range(vals.shape[0]):
            for c in range(tiles):
                row = 32 + 16 * k + r * tiles + c
                pack[row:row + 1, :] = vals[r:r + 1, c * 128:(c + 1) * 128]
    counts = jnp.zeros((1, 128), wide)
    for i in range(N_TILE):
        row = mask[i].astype(wide)
        for c in range(TILE // 128):
            counts += row[:, c * 128:(c + 1) * 128]
    pack[80:81, :] = counts
    for k in range(N_STREAM):
        pz, py, px = (torus_order(coords[d], first_pairing(k, d, core)) for d in (2, 1, 0))
        buf[core, k, pz, py, px] = pack[16 * k:16 * k + 16, :].astype(jnp.bfloat16)
    pl.semaphore_wait(barrier, 7)
    sent = []
    flight = [None] * N_STREAM
    for s in range(6):
        for k in range(N_STREAM):
            if s > 0:
                flight[k].wait_recv()
            flight[k] = gather_send(buf, k, s, me, core, coords, send_sem, recv_sem)
            flight[k].start()
            sent.append(flight[k])
    for k in range(N_STREAM):
        flight[k].wait_recv()
        ref = buf.at[core, k]
        flight[k] = send_copy(ref, ref, side_send.at[k], side_recv.at[k], me + 1 - 2 * core)
        flight[k].start()
        sent.append(flight[k])
    for c in flight:
        c.wait_recv()
    return sent


def gathered_blocks(k):
    order = ((0, 1, 2, 3), (0, 2, 3, 1))
    for core in range(2):
        first = [(core + ((k + (d - k) % 3) // 3) % 2) % 2 for d in range(3)]
        for z in range(4):
            for y in range(4):
                for x in range(4):
                    yield ((z * 4 + y) * 4 + x) * 2 + core, (core, k, order[first[2]][z], order[first[1]][y], order[first[0]][x])


def recv_shape(k, s):
    sizes = [4, 4, 4]
    for q in range(s + 1):
        sizes[(k + q) % 3] //= 2
    return sizes[2], sizes[1], sizes[0]


def reduce_phase(me, core, coords, g, side, res, recv, send_sem, recv_sem, side_send, side_recv):
    sides = []
    for k, (r0, rn) in enumerate(RS_STREAMS):
        c = send_copy(g.at[:, :, :, 1 - core, pl.ds(r0, rn), :], side.at[:, :, :, pl.ds(r0, rn), :], side_send.at[k], side_recv.at[k], me + 1 - 2 * core)
        c.start()
        sides.append(c)

    def at_dim(d, idx):
        full = [slice(None)] * 3
        full[2 - d] = idx
        return tuple(full)

    pending = {}
    for s in range(7):
        for k, (r0, rn) in enumerate(RS_STREAMS):
            rows = pl.ds(r0, rn)
            if s == 0:
                sides[k].wait_recv()
                side[:, :, :, rows, :] += g[:, :, :, core, rows, :]
                cur = side.at[:, :, :, rows, :]
            else:
                q = s - 1
                for c in pending[k, q]:
                    c.wait_recv()
                d, t = link_of(k, q, core)
                v = coords[d]
                prev = side.at[:, :, :, rows, :] if q == 0 else recv[k * 6 + q - 1]
                cur = recv[k * 6 + q]
                if q < 3:
                    mate = torus_partner(v, 1 - t)
                    lo = jnp.minimum(v, mate)
                    hi = jnp.maximum(v, mate)
                    for j, idx in enumerate((lo, hi)):
                        at = at_dim(d, pl.ds(j, 1))
                        cur[at] += prev[at_dim(d, pl.ds(idx, 1))]
                else:
                    mate = torus_partner(v, t)
                    keep = jnp.where(v > mate, 1, 0)
                    cur[...] += prev[at_dim(d, pl.ds(keep, 1))]
            if s == 6:
                res[rows, :] = cur[0, 0, 0]
                continue
            d, t = link_of(k, s, core)
            v = coords[d]
            mate = torus_partner(v, t)
            target = me + (mate - v) * STRIDES[d]
            dst = recv[k * 6 + s]
            copies = []
            if s < 3:
                far = torus_partner(mate, 1 - t)
                lo = jnp.minimum(mate, far)
                hi = jnp.maximum(mate, far)
                for j, idx in enumerate((lo, hi)):
                    c = send_copy(cur.at[at_dim(d, pl.ds(idx, 1))], dst.at[at_dim(d, pl.ds(j, 1))], send_sem.at[k, 2 * s + j], recv_sem.at[k, 2 * s + j], target)
                    c.start()
                    copies.append(c)
            else:
                give = jnp.where(v > mate, 0, 1)
                c = send_copy(cur.at[at_dim(d, pl.ds(give, 1))], dst, send_sem.at[k, 3 + s], recv_sem.at[k, 3 + s], target)
                c.start()
                copies.append(c)
            pending[k, s] = copies
    return [c for copies in pending.values() for c in copies] + sides


def mm(a, b):
    return jnp.dot(a, b, preferred_element_type=jnp.float32)


def mm_nt(a, b):
    return lax.dot_general(a, b, ROW_CONTRACT, preferred_element_type=jnp.float32)


def compute_scratch():
    v = lambda dt, *shape: pltpu.VMEM(shape, dt)
    f32, bf16 = jnp.float32, jnp.bfloat16
    return [
        v(bf16, 2048, 256), v(bf16, 256, 2048),
        v(bf16, 256, 768), v(bf16, 768, 256), v(bf16, 256, 768), v(bf16, 768, 256), v(bf16, 768, 256), v(bf16, 256, 768),
        v(f32, 256, 128), v(f32, 256, 128), v(f32, 1, TILE),
        v(f32, 2048, 256), v(f32, 256, 768), v(f32, 256, 768), v(f32, 768, 256),
        v(f32, 2048, TILE), v(bf16, 2048, TILE), v(bf16, 2048, TILE),
        v(f32, 768, TILE), v(f32, 768, TILE), v(bf16, 768, TILE), v(f32, 256, TILE), v(bf16, 768, TILE), v(bf16, 768, TILE), v(f32, 1536, 128),
    ]


def compute_phase(buf, ids, labels, mask, g1, g2, g, e_s, et_s, wg_s, wgt_s, wu_s, wut_s, wd_s, wdt_s, g1_s, g2_s, loss_s, d_e, d_wg, d_wu, d_wd, logit_s, dl_s, oh_s, sl_s, dp_s, u_s, dh_s, dq_s, dpb_s, stage):
    f32, bf16 = jnp.float32, jnp.bfloat16
    rows = g.reshape(128 * RS_ROWS, 128)
    for j in range(3):
        for dev, at in gathered_blocks(2 + j):
            rows[dev * RS_ROWS + 16 * j:dev * RS_ROWS + 16 * j + 16, :] = buf[at].astype(f32)
    total = jnp.sum(buf[:, 5, :, :, :, 0:16, :].astype(f32))
    for j, (acc, w, wt) in enumerate(((d_wg, wg_s, wgt_s), (d_wu, wu_s, wut_s), (d_wd, wd_s, wdt_s))):
        n = acc.shape[0]
        per, tiles = n // 128, acc.shape[1] // 128
        for c in range(tiles):
            for r in range(per):
                stage[pl.ds(c * n + r, 128, stride=per), :] = rows[pl.ds(16 * j + r * tiles + c, 128, stride=RS_ROWS), :]
            acc[:, c * 128:(c + 1) * 128] = stage[c * n:(c + 1) * n, :]
        w[...] = acc[...].astype(bf16)
        wt[...] = acc[...].T.astype(bf16)
        acc[...] = jnp.zeros_like(acc)
    for half in range(2):
        for dev, at in gathered_blocks(half):
            e_s[16 * dev:16 * dev + 16, 128 * half:128 * half + 128] = buf[at]
        et_s[128 * half:128 * half + 128, :] = e_s[:, 128 * half:128 * half + 128].T
    g1_s[...] = jnp.broadcast_to(g1[...], (128, 256)).T
    g2_s[...] = jnp.broadcast_to(g2[...], (128, 256)).T
    d_e[...] = jnp.zeros_like(d_e)
    loss_s[...] = jnp.zeros_like(loss_s)

    def wide_gain(ref):
        return jnp.concatenate([ref[...]] * (TILE // 128), axis=1)

    def norm(x, gain):
        r = lax.rsqrt(jnp.mean(x * x, axis=0, keepdims=True) + NORM_EPS)
        return (x * r * gain).astype(bf16), r

    def norm_back(x, r, gain, grad):
        sg = grad * gain
        return r * (sg - x * (r * r) * jnp.mean(sg * x, axis=0, keepdims=True))

    def tile_step(i, carry):
        id_row, label_row = ids[i], labels[i]
        coef = mask[i].astype(f32) / total
        for v in range(0, 2048, V_CHUNK):
            vocab = lax.broadcasted_iota(jnp.int32, (V_CHUNK, TILE), 0) + v
            oh_s[v:v + V_CHUNK, :] = jnp.where(vocab == id_row, 1.0, 0.0).astype(bf16)
        x = mm(et_s[...], oh_s[...])
        gain1, gain2 = wide_gain(g1_s), wide_gain(g2_s)
        a, r1 = norm(x, gain1)
        for f in range(0, 768, F_CHUNK):
            sl = slice(f, f + F_CHUNK)
            p = mm(wgt_s[sl, :], a).astype(bf16).astype(f32)
            q = mm(wut_s[sl, :], a).astype(bf16).astype(f32)
            s = jax.nn.sigmoid(p)
            silu = p * s
            sl_s[sl, :] = silu
            u_s[sl, :] = (silu * q).astype(bf16)
            dp_s[sl, :] = q * s * (1.0 + p * (1.0 - s))
        h = (x + mm(wdt_s[...], u_s[...])).astype(bf16).astype(f32)
        hn, r2 = norm(h, gain2)
        top = jnp.full((1, TILE), -jnp.inf, f32)
        for v in range(0, 2048, V_CHUNK):
            part = mm(e_s[v:v + V_CHUNK, :], hn)
            logit_s[v:v + V_CHUNK, :] = part
            top = jnp.maximum(top, jnp.max(part, axis=0, keepdims=True))
        den = jnp.zeros((1, TILE), f32)
        picked = jnp.zeros((1, TILE), f32)
        for v in range(0, 2048, V_CHUNK):
            part = logit_s[v:v + V_CHUNK, :]
            vocab = lax.broadcasted_iota(jnp.int32, (V_CHUNK, TILE), 0) + v
            picked += jnp.sum(jnp.where(vocab == label_row, part, 0.0), axis=0, keepdims=True)
            part = jnp.exp(part - top)
            den += jnp.sum(part, axis=0, keepdims=True)
            logit_s[v:v + V_CHUNK, :] = part
        loss_s[...] += coef * (top + jnp.log(den) - picked)
        scale = coef / den
        for v in range(0, 2048, V_CHUNK):
            vocab = lax.broadcasted_iota(jnp.int32, (V_CHUNK, TILE), 0) + v
            part = logit_s[v:v + V_CHUNK, :] * scale
            dl_s[v:v + V_CHUNK, :] = (part - jnp.where(vocab == label_row, coef, 0.0)).astype(bf16)
        dhn = mm(et_s[...], dl_s[...])
        dh = norm_back(h, r2, gain2, dhn)
        dhb = dh.astype(bf16)
        dh_s[...] = dh
        for f in range(0, 768, F_CHUNK):
            sl = slice(f, f + F_CHUNK)
            du = mm(wd_s[sl, :], dhb)
            dq_s[sl, :] = (du * sl_s[sl, :]).astype(bf16)
            dpb_s[sl, :] = (du * dp_s[sl, :]).astype(bf16)
            d_wd[sl, :] += mm_nt(u_s[sl, :], dhb)
        d_wg[...] += mm_nt(a, dpb_s[...])
        d_wu[...] += mm_nt(a, dq_s[...])
        da = mm(wg_s[...], dpb_s[...]) + mm(wu_s[...], dq_s[...])
        dx = dh_s[...] + norm_back(x, r1, gain1, da)
        hi = dx.astype(bf16)
        rest = dx - hi.astype(f32)
        mid = rest.astype(bf16)
        low = (rest - mid.astype(f32)).astype(bf16)
        for v in range(0, 2048, V_CHUNK):
            sl = slice(v, v + V_CHUNK)
            oh = oh_s[sl, :]
            d_e[sl, :] += mm_nt(dl_s[sl, :], hn) + mm_nt(oh, hi) + mm_nt(oh, mid) + mm_nt(oh, low)
        return carry

    lax.fori_loop(0, N_TILE, tile_step, 0)

    for half in range(2):
        g[:, :, :, :, 16 * half:16 * half + 16, :] = d_e[:, 128 * half:128 * half + 128].reshape(4, 4, 4, 2, 16, 128)
    for base, acc in ((RS_GATE, d_wg), (RS_UP, d_wu), (RS_DOWN, d_wd)):
        n = acc.shape[0]
        per, tiles = n // 128, acc.shape[1] // 128
        for c in range(tiles):
            stage[c * n:(c + 1) * n, :] = acc[:, c * 128:(c + 1) * 128]
            for r in range(per):
                rows[pl.ds(base + r * tiles + c, 128, stride=RS_ROWS), :] = stage[pl.ds(c * n + r, 128, stride=per), :]
    loss = jnp.sum(loss_s[...])
    for r in range(RS_LOSS, RS_ROWS):
        rows[pl.ds(r, 128, stride=RS_ROWS), :] = jnp.full((128, 128), loss, f32)


def whole_kernel(e_hbm, wg_hbm, wu_hbm, wd_hbm, ids_hbm, labels_hbm, mask_hbm, g1_hbm, g2_hbm, loss_ref, e_out, wg_out, wu_out, wd_out, *refs):
    me, core, coords = my_place()
    barrier = greet(me, core, coords)
    n_in = 9
    local = refs[:n_in]
    in_sem = refs[n_in]
    buf, pack, side, res, g = refs[n_in + 1:n_in + 6]
    recv = refs[n_in + 6:n_in + 42]
    ag_send, ag_recv, ag_side_send, ag_side_recv, rs_send, rs_recv, rs_side_send, rs_side_recv = refs[n_in + 42:n_in + 50]
    scratch = refs[n_in + 50:]
    loads = [pltpu.make_async_copy(src, dst, in_sem.at[i]) for i, (src, dst) in enumerate(zip((e_hbm, wg_hbm, wu_hbm, wd_hbm, ids_hbm, labels_hbm, mask_hbm, g1_hbm, g2_hbm), local))]
    for c in loads:
        c.start()
    for c in loads:
        c.wait()
    e_in, wg_in, wu_in, wd_in, ids, labels, mask, g1, g2 = local
    sent = gather_phase(me, core, coords, barrier, (e_in, wg_in, wu_in, wd_in), mask, buf, pack, ag_send, ag_recv, ag_side_send, ag_side_recv)
    compute_phase(buf, ids, labels, mask, g1, g2, g, *scratch)
    sent += reduce_phase(me, core, coords, g, side, res, recv, rs_send, rs_recv, rs_side_send, rs_side_recv)
    loss_ref[...] = res[RS_LOSS:RS_LOSS + 1, :]
    e_out[:, 0:128] = res[0:16, :]
    e_out[:, 128:256] = res[16:32, :]
    for base, ref in ((RS_GATE, wg_out), (RS_UP, wu_out), (RS_DOWN, wd_out)):
        tiles = ref.shape[1] // 128
        for r in range(ref.shape[0]):
            for c in range(tiles):
                row = base + r * tiles + c
                ref[r:r + 1, c * 128:(c + 1) * 128] = res[row:row + 1, :]
    for c in sent:
        c.wait_send()


def whole_step(*args):
    vm = pl.BlockSpec(memory_space=pltpu.VMEM)
    v = lambda dt, *shape: pltpu.VMEM(shape, dt)
    f32 = jnp.float32
    sds = lambda *shape: jax.ShapeDtypeStruct(shape, f32)
    recvs = [v(f32, *recv_shape(k, s), rn, 128) for k, (_, rn) in enumerate(RS_STREAMS) for s in range(6)]
    sem = pltpu.SemaphoreType.DMA
    return pl.pallas_call(
        whole_kernel,
        out_shape=(sds(1, 128), sds(16, 256), sds(2, 768), sds(2, 768), sds(6, 256)),
        in_specs=[pl.BlockSpec(memory_space=pl.ANY)] * 9,
        out_specs=(vm,) * 5,
        scratch_shapes=[
            *[v(a.dtype, *a.shape) for a in args],
            sem((9,)),
            v(jnp.bfloat16, 2, N_STREAM, 4, 4, 4, 16, 128), v(f32, AG_ROWS, 128),
            v(f32, 4, 4, 4, RS_ROWS, 128), v(f32, RS_ROWS, 128), v(f32, 4, 4, 4, 2, RS_ROWS, 128),
            *recvs,
            sem((N_STREAM, 6)), sem((N_STREAM, 6)), sem((N_STREAM,)), sem((N_STREAM,)),
            sem((N_STREAM, 9)), sem((N_STREAM, 9)), sem((N_STREAM,)), sem((N_STREAM,)),
            *compute_scratch(),
        ],
        compiler_params=pltpu.CompilerParams(collective_id=0, has_side_effects=True, vmem_limit_bytes=62 << 20),
        name="whole_step",
    )(*args)


def solution(mesh):
    def device_step(tok_ids, tok_labels, loss_mask, table_shard, gain_mlp, gain_head, gate_shard, up_shard, down_shard):
        tok = lambda t: t.reshape(N_TILE, 1, TILE)
        loss, e_out, wg_out, wu_out, wd_out = whole_step(table_shard, gate_shard, up_shard, down_shard, tok(tok_ids), tok(tok_labels), tok(loss_mask), gain_mlp.reshape(1, 256), gain_head.reshape(1, 256))
        return loss[0, 0], e_out, wg_out, wu_out, wd_out

    row_spec = P("fsdp", None)
    tok_spec = P("fsdp")
    return jax.shard_map(device_step, mesh=mesh, in_specs=(tok_spec, tok_spec, tok_spec, row_spec, P(), P(), row_spec, row_spec, row_spec), out_specs=(P(), row_spec, row_spec, row_spec, row_spec), check_vma=False)
```

```python
import functools

import jax
import jax.numpy as jnp
from jax import lax
from jax.experimental import pallas as pl
from jax.experimental.pallas import tpu as pltpu
from jax.sharding import PartitionSpec as P

NORM_EPS = 1e-6
ROW_CONTRACT = (((1,), (1,)), ((), ()))
MESH = pl.DeviceIdType.MESH
AXIS = "fsdp"
STRIDES = (2, 8, 32)
N_STREAM = 6
AG_ROWS = 96
RS_ROWS = 72
RS_GATE, RS_UP, RS_DOWN, RS_LOSS = 32, 44, 56, 68
RS_STREAMS = tuple((8 * j, 8, j % 6) for j in range(9))
RS_TABLE, RS_WEIGHTS = (0, 1, 2, 3), (4, 5, 6, 7, 8)
N_RS = len(RS_STREAMS)


TILE = 1024
N_TILE = 4096 // TILE
V_CHUNK = 256
F_CHUNK = 384
TG_CHUNK = 1024
EARLY = False


def torus_partner(v, t):
    near = v + 1 - 2 * lax.rem(v, 2)
    far = 3 - v
    return near + t * (far - near)


def my_place():
    me = lax.axis_index(AXIS)
    core = lax.rem(me, 2)
    coords = (lax.rem(lax.div(me, 2), 4), lax.rem(lax.div(me, 8), 4), lax.div(me, 32))
    return me, core, coords


def greet(me, core, coords):
    barrier = pltpu.get_barrier_semaphore()
    pl.semaphore_signal(barrier, inc=1, device_id=(me + 1 - 2 * core,), device_id_type=MESH)
    for d in range(3):
        for t in range(2):
            other = me + (torus_partner(coords[d], t) - coords[d]) * STRIDES[d]
            pl.semaphore_signal(barrier, inc=1, device_id=(other,), device_id_type=MESH)
    return barrier


def link_of(k, s, core):
    return (k + s) % 3, lax.rem(core + ((k + s) // 3) % 2, 2)


def send_copy(src, dst, send_sem, recv_sem, target):
    return pltpu.make_async_remote_copy(src_ref=src, dst_ref=dst, send_sem=send_sem, recv_sem=recv_sem, device_id=(target,), device_id_type=MESH)


def torus_order(v, t):
    return v + t * (min_int(v, 1) * (lax.rem(v, 3) + 1) - v)


def min_int(a, b):
    return jnp.minimum(a, b)


def first_pairing(k, d, core):
    s = (d - k) % 3
    return link_of(k, s, core)[1]


def gather_send(buf, k, s, me, core, coords, send_sem, recv_sem):
    idx = []
    for d in (2, 1, 0):
        done = len([q for q in range(s) if (k + q) % 3 == d])
        p = torus_order(coords[d], first_pairing(k, d, core))
        idx.append((pl.ds(p, 1), pl.ds(2 * lax.div(p, 2), 2), pl.ds(0, 4))[done])
    d, t = link_of(k, s, core)
    target = me + (torus_partner(coords[d], t) - coords[d]) * STRIDES[d]
    ref = buf.at[(core, k, *idx)]
    return send_copy(ref, ref, send_sem.at[k, s], recv_sem.at[k, s], target)


def side_send_half(buf, k, late, me, core, coords, side_send, side_recv):
    d, _ = link_of(k, 5, core)
    p = lax.div(torus_order(coords[d], first_pairing(k, d, core)), 2)
    idx = [pl.ds(0, 4)] * 3
    idx[2 - d] = pl.ds(2 * (p + late * (1 - 2 * p)), 2)
    ref = buf.at[(core, k, *idx)]
    return send_copy(ref, ref, side_send.at[k, late], side_recv.at[k, late], me + 1 - 2 * core)


def gather_phase(me, core, coords, barrier, shards, mask, buf, pack, send_sem, recv_sem, side_send, side_recv):
    cx, cy, cz = coords
    wide = jnp.float32
    e_ref, *w_refs = shards
    pack[0:16, :] = e_ref[:, 0:128].astype(wide)
    pack[16:32, :] = e_ref[:, 128:256].astype(wide)
    pack[32:AG_ROWS, :] = jnp.zeros((AG_ROWS - 32, 128), wide)
    for k, ref in enumerate(w_refs):
        vals = ref[...].astype(wide)
        tiles = vals.shape[1] // 128
        for r in range(vals.shape[0]):
            for c in range(tiles):
                row = 32 + 16 * k + r * tiles + c
                pack[row:row + 1, :] = vals[r:r + 1, c * 128:(c + 1) * 128]
    counts = jnp.zeros((1, 128), wide)
    for i in range(N_TILE):
        row = mask[i].astype(wide)
        for c in range(TILE // 128):
            counts += row[:, c * 128:(c + 1) * 128]
    pack[80:81, :] = counts
    for k in range(N_STREAM):
        pz, py, px = (torus_order(coords[d], first_pairing(k, d, core)) for d in (2, 1, 0))
        buf[core, k, pz, py, px] = pack[16 * k:16 * k + 16, :].astype(jnp.bfloat16)
    pl.semaphore_wait(barrier, 7)
    sent = []
    flight = [None] * N_STREAM
    sides = []
    for s in range(6):
        for k in range(N_STREAM):
            if s > 0:
                flight[k].wait_recv()
            flight[k] = gather_send(buf, k, s, me, core, coords, send_sem, recv_sem)
            flight[k].start()
            sent.append(flight[k])
            if s == 5:
                sides.append(side_send_half(buf, k, 0, me, core, coords, side_send, side_recv))
                sides[-1].start()
    return sent, flight, sides


def gathered_blocks(k):
    order = ((0, 1, 2, 3), (0, 2, 3, 1))
    for core in range(2):
        first = [(core + ((k + (d - k) % 3) // 3) % 2) % 2 for d in range(3)]
        for z in range(4):
            for y in range(4):
                for x in range(4):
                    yield ((z * 4 + y) * 4 + x) * 2 + core, (core, k, order[first[2]][z], order[first[1]][y], order[first[0]][x])


def recv_shape(k, s):
    sizes = [4, 4, 4]
    for q in range(s + 1):
        sizes[(k + q) % 3] //= 2
    return sizes[2], sizes[1], sizes[0]


class Reducer:
    def __init__(self, me, core, coords, g, side, res, recv, send_sem, recv_sem, side_send, side_recv):
        self.me, self.core, self.coords = me, core, coords
        self.g, self.side, self.res, self.recv = g, side, res, recv
        self.sems = (send_sem, recv_sem, side_send, side_recv)
        self.flight = [None] * N_RS
        self.stage = [0] * N_RS
        self.sent = []

    def at_dim(self, d, idx):
        full = [slice(None)] * 3
        full[2 - d] = idx
        return tuple(full)

    def post(self, j, copies):
        for c in copies:
            c.start()
        self.flight[j] = copies
        self.sent += copies

    def advance(self, j):
        me, core, coords = self.me, self.core, self.coords
        send_sem, recv_sem, side_send, side_recv = self.sems
        r0, rn, k = RS_STREAMS[j]
        rows = pl.ds(r0, rn)
        stage = self.stage[j]
        self.stage[j] += 1
        if stage == 0:
            src = self.g.at[:, :, :, 1 - core, rows, :]
            self.post(j, [send_copy(src, self.side.at[:, :, :, rows, :], side_send.at[j], side_recv.at[j], me + 1 - 2 * core)])
            return
        for c in self.flight[j]:
            c.wait_recv()
        if stage == 1:
            self.side[:, :, :, rows, :] += self.g[:, :, :, core, rows, :]
            cur = self.side.at[:, :, :, rows, :]
        else:
            q = stage - 2
            d, t = link_of(k, q, core)
            v = coords[d]
            prev = self.side.at[:, :, :, rows, :] if q == 0 else self.recv[j * 6 + q - 1]
            cur = self.recv[j * 6 + q]
            if q < 3:
                mate = torus_partner(v, 1 - t)
                for i, idx in enumerate((jnp.minimum(v, mate), jnp.maximum(v, mate))):
                    cur[self.at_dim(d, pl.ds(i, 1))] += prev[self.at_dim(d, pl.ds(idx, 1))]
            else:
                mate = torus_partner(v, t)
                keep = jnp.where(v > mate, 1, 0)
                cur[...] += prev[self.at_dim(d, pl.ds(keep, 1))]
        s = stage - 1
        if s == 6:
            self.res[rows, :] = cur[0, 0, 0]
            return
        d, t = link_of(k, s, core)
        v = coords[d]
        mate = torus_partner(v, t)
        target = me + (mate - v) * STRIDES[d]
        dst = self.recv[j * 6 + s]
        if s < 3:
            far = torus_partner(mate, 1 - t)
            copies = [send_copy(cur.at[self.at_dim(d, pl.ds(idx, 1))], dst.at[self.at_dim(d, pl.ds(i, 1))], send_sem.at[j, 2 * s + i], recv_sem.at[j, 2 * s + i], target) for i, idx in enumerate((jnp.minimum(mate, far), jnp.maximum(mate, far)))]
        else:
            give = jnp.where(v > mate, 0, 1)
            copies = [send_copy(cur.at[self.at_dim(d, pl.ds(give, 1))], dst, send_sem.at[j, 3 + s], recv_sem.at[j, 3 + s], target)]
        self.post(j, copies)


def mm(a, b):
    return jnp.dot(a, b, preferred_element_type=jnp.float32)


def mm_nt(a, b):
    return lax.dot_general(a, b, ROW_CONTRACT, preferred_element_type=jnp.float32)


def compute_scratch():
    v = lambda dt, *shape: pltpu.VMEM(shape, dt)
    f32, bf16 = jnp.float32, jnp.bfloat16
    return [
        v(bf16, 2048, 256), v(bf16, 256, 2048),
        v(bf16, 256, 768), v(bf16, 768, 256), v(bf16, 256, 768), v(bf16, 768, 256), v(bf16, 768, 256), v(bf16, 256, 768),
        v(f32, 256, 128), v(f32, 256, 128), v(f32, 1, TILE),
        v(f32, 2048, 256), v(f32, 256, 768), v(f32, 256, 768), v(f32, 768, 256),
        v(f32, 2048, TILE), v(bf16, 2048, TILE), v(bf16, 2048, TILE),
        v(f32, 768, TILE), v(f32, 768, TILE), v(bf16, 768, TILE), v(bf16, 768, TILE), v(bf16, 768, TILE), v(f32, 1536, 128),
        v(f32, 2048, 256), v(bf16, 2048, 128), v(bf16, 256, 2048), v(f32, 8, 2048),
    ]


def compute_phase(buf, ids, labels, mask, g1, g2, g, reducer, ready, e_s, et_s, wg_s, wgt_s, wu_s, wut_s, wd_s, wdt_s, g1_s, g2_s, loss_s, d_e, d_wg, d_wu, d_wd, logit_s, dl_s, oh_s, sl_s, dp_s, u_s, dq_s, dpb_s, stage, s_acc, cnt_s, hn_s, n_s):
    f32, bf16 = jnp.float32, jnp.bfloat16
    g1_s[...] = jnp.broadcast_to(g1[...], (128, 256)).T
    g2_s[...] = jnp.broadcast_to(g2[...], (128, 256)).T
    d_e[...] = jnp.zeros_like(d_e)
    loss_s[...] = jnp.zeros_like(loss_s)
    for half in range(2):
        ready(half)
        for dev, at in gathered_blocks(half):
            e_s[16 * dev:16 * dev + 16, 128 * half:128 * half + 128] = buf[at]
        et_s[128 * half:128 * half + 128, :] = e_s[:, 128 * half:128 * half + 128].T
    s_acc[...] = jnp.zeros_like(s_acc)
    cnt_s[...] = jnp.zeros_like(cnt_s)

    def wide_gain(ref):
        return jnp.concatenate([ref[...]] * (TILE // 128), axis=1)

    def norm(x, gain):
        r = lax.rsqrt(jnp.mean(x * x, axis=0, keepdims=True) + NORM_EPS)
        return (x * r * gain).astype(bf16), r

    def norm_back(x, r, gain, grad):
        sg = grad * gain
        return r * (sg - x * (r * r) * jnp.mean(sg * x, axis=0, keepdims=True))

    def one_hots(i):
        id_row = jnp.where(mask[i] == 1, ids[i], -1)
        label_row = labels[i]
        for v in range(0, 2048, V_CHUNK):
            vocab = lax.broadcasted_iota(jnp.int32, (V_CHUNK, TILE), 0) + v
            oh_s[v:v + V_CHUNK, :] = jnp.where(vocab == id_row, 1.0, 0.0).astype(bf16)
            dl_s[v:v + V_CHUNK, :] = jnp.where(vocab == label_row, 1.0, 0.0).astype(bf16)

    def label_rows(i, carry):
        one_hots(i)
        picked = mm(et_s[...], dl_s[...]).astype(bf16)
        for v in range(0, 2048, TG_CHUNK):
            sl = slice(v, v + TG_CHUNK)
            s_acc[sl, :] += mm_nt(oh_s[sl, :], picked)
        for v in range(0, 2048, V_CHUNK):
            sl = slice(v, v + V_CHUNK)
            count = cnt_s[sl, :]
            for c in range(0, TILE, 128):
                count += oh_s[sl, c:c + 128]
            cnt_s[sl, :] = count
        return carry

    def hidden_rows(i):
        one_hots(i)
        picked = mm(hn_s[...], oh_s[...]).astype(bf16)
        for v in range(0, 2048, TG_CHUNK):
            sl = slice(v, v + TG_CHUNK)
            s_acc[sl, :] += mm_nt(dl_s[sl, :], picked)

    def row_step(j, carry):
        at = pl.ds(pl.multiple_of(j * TILE, TILE), TILE)
        x = et_s[:, at].astype(f32)
        label_sum = s_acc[at, :].T
        n_row = n_s[0:1, at]
        gain1, gain2 = wide_gain(g1_s), wide_gain(g2_s)
        a, r1 = norm(x, gain1)
        for f in range(0, 768, F_CHUNK):
            sl = slice(f, f + F_CHUNK)
            p = mm(wgt_s[sl, :], a).astype(bf16).astype(f32)
            q = mm(wut_s[sl, :], a).astype(bf16).astype(f32)
            s = jax.nn.sigmoid(p)
            silu = p * s
            sl_s[sl, :] = silu
            u_s[sl, :] = (silu * q).astype(bf16)
            dp_s[sl, :] = q * (s + silu * (1.0 - s))
        h = (x + mm(wdt_s[...], u_s[...])).astype(bf16).astype(f32)
        hn, r2 = norm(h, gain2)
        hn_s[:, at] = hn
        top = jnp.full((1, TILE), -jnp.inf, f32)
        for v in range(0, 2048, V_CHUNK):
            part = mm(e_s[v:v + V_CHUNK, :], hn)
            logit_s[v:v + V_CHUNK, :] = part
            top = jnp.maximum(top, jnp.max(part, axis=0, keepdims=True))
        den = jnp.zeros((1, TILE), f32)
        for v in range(0, 2048, V_CHUNK):
            part = jnp.exp(logit_s[v:v + V_CHUNK, :] - top)
            den += jnp.sum(part, axis=0, keepdims=True)
            logit_s[v:v + V_CHUNK, :] = part
        picked = jnp.sum(hn.astype(f32) * label_sum, axis=0, keepdims=True)
        loss_s[...] += coef * (n_row * (top + jnp.log(den)) - picked)
        scale = coef * n_row / den
        for v in range(0, 2048, V_CHUNK):
            dl_s[v:v + V_CHUNK, :] = (logit_s[v:v + V_CHUNK, :] * scale).astype(bf16)
        dhn = mm(et_s[...], dl_s[...]) - coef * label_sum
        dh = norm_back(h, r2, gain2, dhn)
        dhb = dh.astype(bf16)
        for f in range(0, 768, F_CHUNK):
            sl = slice(f, f + F_CHUNK)
            du = mm(wd_s[sl, :], dhb)
            dq_s[sl, :] = (du * sl_s[sl, :]).astype(bf16)
            dpb_s[sl, :] = (du * dp_s[sl, :]).astype(bf16)
            d_wd[sl, :] += mm_nt(u_s[sl, :], dhb)
        d_wg[...] += mm_nt(a, dpb_s[...])
        d_wu[...] += mm_nt(a, dq_s[...])
        da = mm(wg_s[...], dpb_s[...]) + mm(wu_s[...], dq_s[...])
        dx = dh + norm_back(x, r1, gain1, da)
        for v in range(0, 2048, TG_CHUNK):
            sl = slice(v, v + TG_CHUNK)
            d_e[sl, :] += mm_nt(dl_s[sl, :], hn)
        d_e[at, :] += dx.T
        return carry

    lax.fori_loop(0, N_TILE, label_rows, 0)
    n_s[...] = mm_nt(jnp.ones((8, 128), bf16), cnt_s[...])
    rows = g.reshape(128 * RS_ROWS, 128)
    for j in range(3):
        ready(2 + j)
        for dev, at in gathered_blocks(2 + j):
            rows[dev * RS_ROWS + 16 * j:dev * RS_ROWS + 16 * j + 16, :] = buf[at].astype(f32)
    ready(5)
    total = jnp.sum(buf[:, 5, :, :, :, 0:16, :].astype(f32))
    for j, (acc, w, wt) in enumerate(((d_wg, wg_s, wgt_s), (d_wu, wu_s, wut_s), (d_wd, wd_s, wdt_s))):
        n = acc.shape[0]
        per, tiles = n // 128, acc.shape[1] // 128
        for c in range(tiles):
            for r in range(per):
                stage[pl.ds(c * n + r, 128, stride=per), :] = rows[pl.ds(16 * j + r * tiles + c, 128, stride=RS_ROWS), :]
            acc[:, c * 128:(c + 1) * 128] = stage[c * n:(c + 1) * n, :]
        w[...] = acc[...].astype(bf16)
        wt[...] = acc[...].T.astype(bf16)
        acc[...] = jnp.zeros_like(acc)
    coef = 1.0 / total
    lax.fori_loop(0, 2048 // TILE, row_step, 0)

    for base, acc in ((RS_GATE, d_wg), (RS_UP, d_wu), (RS_DOWN, d_wd)):
        n = acc.shape[0]
        per, tiles = n // 128, acc.shape[1] // 128
        for c in range(tiles):
            stage[c * n:(c + 1) * n, :] = acc[:, c * 128:(c + 1) * 128]
            for r in range(per):
                rows[pl.ds(base + r * tiles + c, 128, stride=RS_ROWS), :] = stage[pl.ds(c * n + r, 128, stride=per), :]
    loss = jnp.sum(loss_s[...])
    for r in range(RS_LOSS, RS_ROWS):
        rows[pl.ds(r, 128, stride=RS_ROWS), :] = jnp.full((128, 128), loss, f32)
    s_acc[...] = jnp.zeros_like(s_acc)
    if EARLY:
        for j in RS_WEIGHTS:
            reducer.advance(j)
        for i in range(N_TILE):
            hidden_rows(i)
            for j in RS_WEIGHTS:
                reducer.advance(j)
    else:
        lax.fori_loop(0, N_TILE, lambda i, c: (hidden_rows(i), c)[1], 0)
    for half in range(2):
        cols = slice(128 * half, 128 * half + 128)
        g[:, :, :, :, 16 * half:16 * half + 16, :] = (d_e[:, cols] - coef * s_acc[:, cols]).reshape(4, 4, 4, 2, 16, 128)
    while min(reducer.stage) < 8:
        for j in RS_TABLE + RS_WEIGHTS:
            if reducer.stage[j] < 8:
                reducer.advance(j)


def whole_kernel(*refs):
    me, core, coords = my_place()
    barrier = greet(me, core, coords)
    n_in = 9
    sources, res_out, local, in_sem = refs[:n_in], refs[n_in], refs[n_in + 1:2 * n_in + 1], refs[2 * n_in + 1]
    refs = refs[2 * n_in + 2:]
    buf, pack, side, g = refs[:4]
    recv = refs[4:4 + 6 * N_RS]
    ag_send, ag_recv, ag_side_send, ag_side_recv = refs[4 + 6 * N_RS:8 + 6 * N_RS]
    rs_sems = refs[8 + 6 * N_RS:12 + 6 * N_RS]
    scratch = refs[12 + 6 * N_RS:]
    loads = [pltpu.make_async_copy(src, dst, in_sem.at[i]) for i, (src, dst) in enumerate(zip(sources, local))]
    for c in loads:
        c.start()
    for c in loads:
        c.wait()
    *shards, ids, labels, mask, g1, g2 = local
    sent, flight, sides = gather_phase(me, core, coords, barrier, shards, mask, buf, pack, ag_send, ag_recv, ag_side_send, ag_side_recv)
    late = []
    for k in range(N_STREAM):
        flight[k].wait_recv()
        late.append(side_send_half(buf, k, 1, me, core, coords, ag_side_send, ag_side_recv))
        late[k].start()

    def ready(k):
        sides[k].wait_recv()
        late[k].wait_recv()

    reducer = Reducer(me, core, coords, g, side, res_out, recv, *rs_sems)
    compute_phase(buf, ids, labels, mask, g1, g2, g, reducer, ready, *scratch)
    for c in sent + sides + late + reducer.sent:
        c.wait_send()


def whole_step(*args):
    vm = pl.BlockSpec(memory_space=pltpu.VMEM)
    v = lambda dt, *shape: pltpu.VMEM(shape, dt)
    f32 = jnp.float32
    recvs = [v(f32, *recv_shape(k, s), rn, 128) for _, rn, k in RS_STREAMS for s in range(6)]
    sem = pltpu.SemaphoreType.DMA
    return pl.pallas_call(
        whole_kernel,
        out_shape=jax.ShapeDtypeStruct((RS_ROWS, 128), f32),
        in_specs=[pl.BlockSpec(memory_space=pl.ANY)] * 9,
        out_specs=vm,
        scratch_shapes=[
            *[v(a.dtype, *a.shape) for a in args],
            sem((9,)),
            v(jnp.bfloat16, 2, N_STREAM, 4, 4, 4, 16, 128), v(f32, AG_ROWS, 128),
            v(f32, 4, 4, 4, RS_ROWS, 128), v(f32, 4, 4, 4, 2, RS_ROWS, 128),
            *recvs,
            sem((N_STREAM, 6)), sem((N_STREAM, 6)), sem((N_STREAM, 2)), sem((N_STREAM, 2)),
            sem((N_RS, 9)), sem((N_RS, 9)), sem((N_RS,)), sem((N_RS,)),
            *compute_scratch(),
        ],
        compiler_params=pltpu.CompilerParams(collective_id=0, has_side_effects=True, vmem_limit_bytes=67043328),
        name="whole_step",
    )(*args)


def split_kernel(res, loss_ref, e_out, wg_out, wu_out, wd_out):
    loss_ref[0, 0] = res[RS_LOSS, 0]
    e_out[:, 0:128] = res[0:16, :]
    e_out[:, 128:256] = res[16:32, :]
    for base, ref in ((RS_GATE, wg_out), (RS_UP, wu_out), (RS_DOWN, wd_out)):
        tiles = ref.shape[1] // 128
        for r in range(ref.shape[0]):
            for c in range(tiles):
                row = base + r * tiles + c
                ref[r:r + 1, c * 128:(c + 1) * 128] = res[row:row + 1, :]


def split_result(res):
    vm = pl.BlockSpec(memory_space=pltpu.VMEM)
    sds = lambda *shape: jax.ShapeDtypeStruct(shape, jnp.float32)
    return pl.pallas_call(
        split_kernel,
        out_shape=(sds(1, 1), sds(16, 256), sds(2, 768), sds(2, 768), sds(6, 256)),
        in_specs=[vm],
        out_specs=(pl.BlockSpec(memory_space=pltpu.SMEM), vm, vm, vm, vm),
        compiler_params=pltpu.CompilerParams(vmem_limit_bytes=1 << 20),
        name="split_result",
    )(res)


def solution(mesh):
    def device_step(tok_ids, tok_labels, loss_mask, table_shard, gain_mlp, gain_head, gate_shard, up_shard, down_shard):
        tok = lambda t: t.reshape(N_TILE, 1, TILE)
        loss, e_out, wg_out, wu_out, wd_out = split_result(whole_step(table_shard, gate_shard, up_shard, down_shard, tok(tok_ids), tok(tok_labels), tok(loss_mask), gain_mlp.reshape(1, 256), gain_head.reshape(1, 256)))
        return loss[0, 0], e_out, wg_out, wu_out, wd_out

    row_spec = P("fsdp", None)
    tok_spec = P("fsdp")
    return jax.shard_map(device_step, mesh=mesh, in_specs=(tok_spec, tok_spec, tok_spec, row_spec, P(), P(), row_spec, row_spec, row_spec), out_specs=(P(), row_spec, row_spec, row_spec, row_spec), check_vma=False)
```

```python
import functools

import jax
import jax.numpy as jnp
from jax import lax
from jax.experimental import pallas as pl
from jax.experimental.pallas import tpu as pltpu
from jax.sharding import PartitionSpec as P

NORM_EPS = 1e-6
ROW_CONTRACT = (((1,), (1,)), ((), ()))
MESH = pl.DeviceIdType.MESH
AXIS = "fsdp"
STRIDES = (2, 8, 32)
N_STREAM = 6
AG_ROWS = 96
RS_ROWS = 72
RS_GATE, RS_UP, RS_DOWN, RS_LOSS = 32, 44, 56, 68
RS_STREAMS = tuple((8 * j, 8, j % 6) for j in range(9))
RS_TABLE, RS_WEIGHTS = (0, 1, 2, 3), (4, 5, 6, 7, 8)
N_RS = len(RS_STREAMS)


TILE = 1024
N_TILE = 4096 // TILE
V_CHUNK = 256
F_CHUNK = 384
TG_CHUNK = 1024
EARLY = False


def torus_partner(v, t):
    near = v + 1 - 2 * lax.rem(v, 2)
    far = 3 - v
    return near + t * (far - near)


def my_place():
    me = lax.axis_index(AXIS)
    core = lax.rem(me, 2)
    coords = (lax.rem(lax.div(me, 2), 4), lax.rem(lax.div(me, 8), 4), lax.div(me, 32))
    return me, core, coords


def greet(me, core, coords):
    barrier = pltpu.get_barrier_semaphore()
    pl.semaphore_signal(barrier, inc=1, device_id=(me + 1 - 2 * core,), device_id_type=MESH)
    for d in range(3):
        for t in range(2):
            other = me + (torus_partner(coords[d], t) - coords[d]) * STRIDES[d]
            pl.semaphore_signal(barrier, inc=1, device_id=(other,), device_id_type=MESH)
    return barrier


def link_of(k, s, core):
    return (k + s) % 3, lax.rem(core + ((k + s) // 3) % 2, 2)


def send_copy(src, dst, send_sem, recv_sem, target):
    return pltpu.make_async_remote_copy(src_ref=src, dst_ref=dst, send_sem=send_sem, recv_sem=recv_sem, device_id=(target,), device_id_type=MESH)


def torus_order(v, t):
    return v + t * (min_int(v, 1) * (lax.rem(v, 3) + 1) - v)


def min_int(a, b):
    return jnp.minimum(a, b)


def first_pairing(k, d, core):
    s = (d - k) % 3
    return link_of(k, s, core)[1]


def gather_send(buf, k, s, me, core, coords, send_sem, recv_sem):
    idx = []
    for d in (2, 1, 0):
        done = len([q for q in range(s) if (k + q) % 3 == d])
        p = torus_order(coords[d], first_pairing(k, d, core))
        idx.append((pl.ds(p, 1), pl.ds(2 * lax.div(p, 2), 2), pl.ds(0, 4))[done])
    d, t = link_of(k, s, core)
    target = me + (torus_partner(coords[d], t) - coords[d]) * STRIDES[d]
    ref = buf.at[(core, k, *idx)]
    return send_copy(ref, ref, send_sem.at[k, s], recv_sem.at[k, s], target)


def side_send_half(buf, k, late, me, core, coords, side_send, side_recv):
    d, _ = link_of(k, 5, core)
    p = lax.div(torus_order(coords[d], first_pairing(k, d, core)), 2)
    idx = [pl.ds(0, 4)] * 3
    idx[2 - d] = pl.ds(2 * (p + late * (1 - 2 * p)), 2)
    ref = buf.at[(core, k, *idx)]
    return send_copy(ref, ref, side_send.at[k, late], side_recv.at[k, late], me + 1 - 2 * core)


def gather_phase(me, core, coords, barrier, shards, mask, buf, pack, send_sem, recv_sem, side_send, side_recv):
    cx, cy, cz = coords
    wide = jnp.float32
    e_ref, *w_refs = shards
    pack[0:16, :] = e_ref[:, 0:128].astype(wide)
    pack[16:32, :] = e_ref[:, 128:256].astype(wide)
    pack[32:AG_ROWS, :] = jnp.zeros((AG_ROWS - 32, 128), wide)
    for k, ref in enumerate(w_refs):
        vals = ref[...].astype(wide)
        tiles = vals.shape[1] // 128
        for r in range(vals.shape[0]):
            for c in range(tiles):
                row = 32 + 16 * k + r * tiles + c
                pack[row:row + 1, :] = vals[r:r + 1, c * 128:(c + 1) * 128]
    counts = jnp.zeros((1, 128), wide)
    for i in range(N_TILE):
        row = mask[i].astype(wide)
        for c in range(TILE // 128):
            counts += row[:, c * 128:(c + 1) * 128]
    pack[80:81, :] = counts
    for k in range(N_STREAM):
        pz, py, px = (torus_order(coords[d], first_pairing(k, d, core)) for d in (2, 1, 0))
        buf[core, k, pz, py, px] = pack[16 * k:16 * k + 16, :].astype(jnp.bfloat16)
    pl.semaphore_wait(barrier, 7)
    sent = []
    flight = [None] * N_STREAM
    sides = []
    for s in range(6):
        for k in range(N_STREAM):
            if s > 0:
                flight[k].wait_recv()
            flight[k] = gather_send(buf, k, s, me, core, coords, send_sem, recv_sem)
            flight[k].start()
            sent.append(flight[k])
            if s == 5:
                sides.append(side_send_half(buf, k, 0, me, core, coords, side_send, side_recv))
                sides[-1].start()
    return sent, flight, sides


def gathered_blocks(k):
    order = ((0, 1, 2, 3), (0, 2, 3, 1))
    for core in range(2):
        first = [(core + ((k + (d - k) % 3) // 3) % 2) % 2 for d in range(3)]
        for z in range(4):
            for y in range(4):
                for x in range(4):
                    yield ((z * 4 + y) * 4 + x) * 2 + core, (core, k, order[first[2]][z], order[first[1]][y], order[first[0]][x])


def recv_shape(k, s):
    sizes = [4, 4, 4]
    for q in range(s + 1):
        sizes[(k + q) % 3] //= 2
    return sizes[2], sizes[1], sizes[0]


class Reducer:
    def __init__(self, me, core, coords, g, side, res, recv, send_sem, recv_sem, side_send, side_recv):
        self.me, self.core, self.coords = me, core, coords
        self.g, self.side, self.res, self.recv = g, side, res, recv
        self.sems = (send_sem, recv_sem, side_send, side_recv)
        self.flight = [None] * N_RS
        self.stage = [0] * N_RS
        self.sent = []

    def at_dim(self, d, idx):
        full = [slice(None)] * 3
        full[2 - d] = idx
        return tuple(full)

    def post(self, j, copies):
        for c in copies:
            c.start()
        self.flight[j] = copies
        self.sent += copies

    def advance(self, j):
        me, core, coords = self.me, self.core, self.coords
        send_sem, recv_sem, side_send, side_recv = self.sems
        r0, rn, k = RS_STREAMS[j]
        rows = pl.ds(r0, rn)
        stage = self.stage[j]
        self.stage[j] += 1
        if stage == 0:
            src = self.g.at[:, :, :, 1 - core, rows, :]
            self.post(j, [send_copy(src, self.side.at[:, :, :, rows, :], side_send.at[j], side_recv.at[j], me + 1 - 2 * core)])
            return
        for c in self.flight[j]:
            c.wait_recv()
        if stage == 1:
            self.side[:, :, :, rows, :] += self.g[:, :, :, core, rows, :]
            cur = self.side.at[:, :, :, rows, :]
        else:
            q = stage - 2
            d, t = link_of(k, q, core)
            v = coords[d]
            prev = self.side.at[:, :, :, rows, :] if q == 0 else self.recv[j * 6 + q - 1]
            cur = self.recv[j * 6 + q]
            if q < 3:
                mate = torus_partner(v, 1 - t)
                for i, idx in enumerate((jnp.minimum(v, mate), jnp.maximum(v, mate))):
                    cur[self.at_dim(d, pl.ds(i, 1))] += prev[self.at_dim(d, pl.ds(idx, 1))]
            else:
                mate = torus_partner(v, t)
                keep = jnp.where(v > mate, 1, 0)
                cur[...] += prev[self.at_dim(d, pl.ds(keep, 1))]
        s = stage - 1
        if s == 6:
            self.res[rows, :] = cur[0, 0, 0]
            return
        d, t = link_of(k, s, core)
        v = coords[d]
        mate = torus_partner(v, t)
        target = me + (mate - v) * STRIDES[d]
        dst = self.recv[j * 6 + s]
        if s < 3:
            far = torus_partner(mate, 1 - t)
            copies = [send_copy(cur.at[self.at_dim(d, pl.ds(idx, 1))], dst.at[self.at_dim(d, pl.ds(i, 1))], send_sem.at[j, 2 * s + i], recv_sem.at[j, 2 * s + i], target) for i, idx in enumerate((jnp.minimum(mate, far), jnp.maximum(mate, far)))]
        else:
            give = jnp.where(v > mate, 0, 1)
            copies = [send_copy(cur.at[self.at_dim(d, pl.ds(give, 1))], dst, send_sem.at[j, 3 + s], recv_sem.at[j, 3 + s], target)]
        self.post(j, copies)


def mm(a, b):
    return jnp.dot(a, b, preferred_element_type=jnp.float32)


def mm_nt(a, b):
    return lax.dot_general(a, b, ROW_CONTRACT, preferred_element_type=jnp.float32)


def compute_scratch():
    v = lambda dt, *shape: pltpu.VMEM(shape, dt)
    f32, bf16 = jnp.float32, jnp.bfloat16
    return [
        v(bf16, 2048, 256), v(bf16, 256, 2048),
        v(bf16, 256, 768), v(bf16, 768, 256), v(bf16, 256, 768), v(bf16, 768, 256), v(bf16, 768, 256), v(bf16, 256, 768),
        v(f32, 256, 128), v(f32, 256, 128), v(f32, 1, TILE),
        v(f32, 2048, 256), v(f32, 256, 768), v(f32, 256, 768), v(f32, 768, 256),
        v(f32, 2048, TILE), v(bf16, 2048, TILE), v(bf16, 2048, TILE),
        v(f32, 768, TILE), v(f32, 768, TILE), v(bf16, 768, TILE), v(bf16, 768, TILE), v(bf16, 768, TILE), v(f32, 1536, 128),
        v(f32, 2048, 256), v(bf16, 2048, 128), v(bf16, 256, 2048), v(f32, 8, 2048),
        v(f32, 1024, 256), v(f32, 8, 1024),
    ]


def compute_phase(buf, ids, labels, mask, g1, g2, g, reducer, ready, core, to_sibling, e_s, et_s, wg_s, wgt_s, wu_s, wut_s, wd_s, wdt_s, g1_s, g2_s, loss_s, d_e, d_wg, d_wu, d_wd, logit_s, dl_s, oh_s, sl_s, dp_s, u_s, dq_s, dpb_s, stage, s_acc, cnt_s, hn_s, n_s, s_in, n_in):
    f32, bf16 = jnp.float32, jnp.bfloat16
    g1_s[...] = jnp.broadcast_to(g1[...], (128, 256)).T
    g2_s[...] = jnp.broadcast_to(g2[...], (128, 256)).T
    d_e[...] = jnp.zeros_like(d_e)
    loss_s[...] = jnp.zeros_like(loss_s)
    for half in range(2):
        ready(half)
        for dev, place in gathered_blocks(half):
            e_s[16 * dev:16 * dev + 16, 128 * half:128 * half + 128] = buf[place]
        et_s[128 * half:128 * half + 128, :] = e_s[:, 128 * half:128 * half + 128].T
    s_acc[...] = jnp.zeros_like(s_acc)
    cnt_s[...] = jnp.zeros_like(cnt_s)

    def wide_gain(ref):
        return jnp.concatenate([ref[...]] * (TILE // 128), axis=1)

    def norm(x, gain):
        r = lax.rsqrt(jnp.mean(x * x, axis=0, keepdims=True) + NORM_EPS)
        return (x * r * gain).astype(bf16), r

    def norm_back(x, r, gain, grad):
        sg = grad * gain
        return r * (sg - x * (r * r) * jnp.mean(sg * x, axis=0, keepdims=True))

    def one_hots(i):
        id_row = jnp.where(mask[i] == 1, ids[i], -1)
        label_row = labels[i]
        for v in range(0, 2048, V_CHUNK):
            vocab = lax.broadcasted_iota(jnp.int32, (V_CHUNK, TILE), 0) + v
            oh_s[v:v + V_CHUNK, :] = jnp.where(vocab == id_row, 1.0, 0.0).astype(bf16)
            dl_s[v:v + V_CHUNK, :] = jnp.where(vocab == label_row, 1.0, 0.0).astype(bf16)

    def label_rows(i, carry):
        one_hots(i)
        picked = mm(et_s[...], dl_s[...]).astype(bf16)
        for v in range(0, 2048, TG_CHUNK):
            sl = slice(v, v + TG_CHUNK)
            s_acc[sl, :] += mm_nt(oh_s[sl, :], picked)
        for v in range(0, 2048, V_CHUNK):
            sl = slice(v, v + V_CHUNK)
            count = cnt_s[sl, :]
            for c in range(0, TILE, 128):
                count += oh_s[sl, c:c + 128]
            cnt_s[sl, :] = count
        return carry

    def hidden_rows(i):
        one_hots(i)
        picked = mm(hn_s[...], oh_s[...]).astype(bf16)
        for v in range(0, 2048, TG_CHUNK):
            sl = slice(v, v + TG_CHUNK)
            s_acc[sl, :] += mm_nt(dl_s[sl, :], picked)

    def row_step():
        x = et_s[:, at].astype(f32)
        label_sum = s_acc[at, :].T
        n_row = n_s[0:1, at]
        gain1, gain2 = wide_gain(g1_s), wide_gain(g2_s)
        a, r1 = norm(x, gain1)
        for f in range(0, 768, F_CHUNK):
            sl = slice(f, f + F_CHUNK)
            p = mm(wgt_s[sl, :], a).astype(bf16).astype(f32)
            q = mm(wut_s[sl, :], a).astype(bf16).astype(f32)
            s = jax.nn.sigmoid(p)
            silu = p * s
            sl_s[sl, :] = silu
            u_s[sl, :] = (silu * q).astype(bf16)
            dp_s[sl, :] = q * (s + silu * (1.0 - s))
        h = (x + mm(wdt_s[...], u_s[...])).astype(bf16).astype(f32)
        hn, r2 = norm(h, gain2)
        hn_s[:, at] = hn
        hidden.start()
        top = jnp.full((1, TILE), -jnp.inf, f32)
        for v in range(0, 2048, V_CHUNK):
            part = mm(e_s[v:v + V_CHUNK, :], hn)
            logit_s[v:v + V_CHUNK, :] = part
            top = jnp.maximum(top, jnp.max(part, axis=0, keepdims=True))
        den = jnp.zeros((1, TILE), f32)
        for v in range(0, 2048, V_CHUNK):
            part = jnp.exp(logit_s[v:v + V_CHUNK, :] - top)
            den += jnp.sum(part, axis=0, keepdims=True)
            logit_s[v:v + V_CHUNK, :] = part
        picked = jnp.sum(hn.astype(f32) * label_sum, axis=0, keepdims=True)
        loss_s[...] += coef * (n_row * (top + jnp.log(den)) - picked)
        scale = coef * n_row / den
        for v in range(0, 2048, V_CHUNK):
            dl_s[v:v + V_CHUNK, :] = (logit_s[v:v + V_CHUNK, :] * scale).astype(bf16)
        dhn = mm(et_s[...], dl_s[...]) - coef * label_sum
        dh = norm_back(h, r2, gain2, dhn)
        dhb = dh.astype(bf16)
        for f in range(0, 768, F_CHUNK):
            sl = slice(f, f + F_CHUNK)
            du = mm(wd_s[sl, :], dhb)
            dq_s[sl, :] = (du * sl_s[sl, :]).astype(bf16)
            dpb_s[sl, :] = (du * dp_s[sl, :]).astype(bf16)
            d_wd[sl, :] += mm_nt(u_s[sl, :], dhb)
        d_wg[...] += mm_nt(a, dpb_s[...])
        d_wu[...] += mm_nt(a, dq_s[...])
        da = mm(wg_s[...], dpb_s[...]) + mm(wu_s[...], dq_s[...])
        dx = dh + norm_back(x, r1, gain1, da)
        for v in range(0, 2048, TG_CHUNK):
            sl = slice(v, v + TG_CHUNK)
            d_e[sl, :] += mm_nt(dl_s[sl, :], hn)
        d_e[at, :] += dx.T

    lax.fori_loop(0, N_TILE, label_rows, 0)
    n_s[...] = mm_nt(jnp.ones((8, 128), bf16), cnt_s[...])
    at = pl.ds(pl.multiple_of(core * 1024, 1024), 1024)
    away = pl.ds(pl.multiple_of((1 - core) * 1024, 1024), 1024)
    sums = [to_sibling(0, s_acc.at[away, :], s_in), to_sibling(1, n_s.at[:, away], n_in)]
    for c in sums:
        c.start()
    rows = g.reshape(128 * RS_ROWS, 128)
    for j in range(3):
        ready(2 + j)
        for dev, place in gathered_blocks(2 + j):
            rows[dev * RS_ROWS + 16 * j:dev * RS_ROWS + 16 * j + 16, :] = buf[place].astype(f32)
    ready(5)
    total = jnp.sum(buf[:, 5, :, :, :, 0:16, :].astype(f32))
    for j, (acc, w, wt) in enumerate(((d_wg, wg_s, wgt_s), (d_wu, wu_s, wut_s), (d_wd, wd_s, wdt_s))):
        n = acc.shape[0]
        per, tiles = n // 128, acc.shape[1] // 128
        for c in range(tiles):
            for r in range(per):
                stage[pl.ds(c * n + r, 128, stride=per), :] = rows[pl.ds(16 * j + r * tiles + c, 128, stride=RS_ROWS), :]
            acc[:, c * 128:(c + 1) * 128] = stage[c * n:(c + 1) * n, :]
        w[...] = acc[...].astype(bf16)
        wt[...] = acc[...].T.astype(bf16)
        acc[...] = jnp.zeros_like(acc)
    coef = 1.0 / total
    for c in sums:
        c.wait_recv()
    s_acc[at, :] += s_in[...]
    n_s[:, at] += n_in[...]
    hidden = to_sibling(2, hn_s.at[:, at], hn_s.at[:, at])
    row_step()

    for base, acc in ((RS_GATE, d_wg), (RS_UP, d_wu), (RS_DOWN, d_wd)):
        n = acc.shape[0]
        per, tiles = n // 128, acc.shape[1] // 128
        for c in range(tiles):
            stage[c * n:(c + 1) * n, :] = acc[:, c * 128:(c + 1) * 128]
            for r in range(per):
                rows[pl.ds(base + r * tiles + c, 128, stride=RS_ROWS), :] = stage[pl.ds(c * n + r, 128, stride=per), :]
    loss = jnp.sum(loss_s[...])
    for r in range(RS_LOSS, RS_ROWS):
        rows[pl.ds(r, 128, stride=RS_ROWS), :] = jnp.full((128, 128), loss, f32)
    for c in sums:
        c.wait_send()
    s_acc[...] = jnp.zeros_like(s_acc)
    hidden.wait()
    if EARLY:
        for j in RS_WEIGHTS:
            reducer.advance(j)
        for i in range(N_TILE):
            hidden_rows(i)
            for j in RS_WEIGHTS:
                reducer.advance(j)
    else:
        lax.fori_loop(0, N_TILE, lambda i, c: (hidden_rows(i), c)[1], 0)
    for half in range(2):
        cols = slice(128 * half, 128 * half + 128)
        g[:, :, :, :, 16 * half:16 * half + 16, :] = (d_e[:, cols] - coef * s_acc[:, cols]).reshape(4, 4, 4, 2, 16, 128)
    while min(reducer.stage) < 8:
        for j in RS_TABLE + RS_WEIGHTS:
            if reducer.stage[j] < 8:
                reducer.advance(j)


def whole_kernel(*refs):
    me, core, coords = my_place()
    barrier = greet(me, core, coords)
    n_in = 9
    sources, res_out, local, in_sem = refs[:n_in], refs[n_in], refs[n_in + 1:2 * n_in + 1], refs[2 * n_in + 1]
    refs = refs[2 * n_in + 2:]
    buf, pack, side, g = refs[:4]
    recv = refs[4:4 + 6 * N_RS]
    ag_send, ag_recv, ag_side_send, ag_side_recv = refs[4 + 6 * N_RS:8 + 6 * N_RS]
    rs_sems = refs[8 + 6 * N_RS:12 + 6 * N_RS]
    pair_sems = refs[12 + 6 * N_RS:14 + 6 * N_RS]
    scratch = refs[14 + 6 * N_RS:]
    loads = [pltpu.make_async_copy(src, dst, in_sem.at[i]) for i, (src, dst) in enumerate(zip(sources, local))]
    for c in loads:
        c.start()
    for c in loads:
        c.wait()
    *shards, ids, labels, mask, g1, g2 = local
    sent, flight, sides = gather_phase(me, core, coords, barrier, shards, mask, buf, pack, ag_send, ag_recv, ag_side_send, ag_side_recv)
    late = []
    for k in range(N_STREAM):
        flight[k].wait_recv()
        late.append(side_send_half(buf, k, 1, me, core, coords, ag_side_send, ag_side_recv))
        late[k].start()

    def ready(k):
        sides[k].wait_recv()
        late[k].wait_recv()

    reducer = Reducer(me, core, coords, g, side, res_out, recv, *rs_sems)

    def to_sibling(i, src, dst):
        return send_copy(src, dst, pair_sems[0].at[i], pair_sems[1].at[i], me + 1 - 2 * core)

    compute_phase(buf, ids, labels, mask, g1, g2, g, reducer, ready, core, to_sibling, *scratch)
    for c in sent + sides + late + reducer.sent:
        c.wait_send()


def whole_step(*args):
    vm = pl.BlockSpec(memory_space=pltpu.VMEM)
    v = lambda dt, *shape: pltpu.VMEM(shape, dt)
    f32 = jnp.float32
    recvs = [v(f32, *recv_shape(k, s), rn, 128) for _, rn, k in RS_STREAMS for s in range(6)]
    sem = pltpu.SemaphoreType.DMA
    return pl.pallas_call(
        whole_kernel,
        out_shape=jax.ShapeDtypeStruct((RS_ROWS, 128), f32),
        in_specs=[pl.BlockSpec(memory_space=pl.ANY)] * 9,
        out_specs=vm,
        scratch_shapes=[
            *[v(a.dtype, *a.shape) for a in args],
            sem((9,)),
            v(jnp.bfloat16, 2, N_STREAM, 4, 4, 4, 16, 128), v(f32, AG_ROWS, 128),
            v(f32, 4, 4, 4, RS_ROWS, 128), v(f32, 4, 4, 4, 2, RS_ROWS, 128),
            *recvs,
            sem((N_STREAM, 6)), sem((N_STREAM, 6)), sem((N_STREAM, 2)), sem((N_STREAM, 2)),
            sem((N_RS, 9)), sem((N_RS, 9)), sem((N_RS,)), sem((N_RS,)), sem((3,)), sem((3,)),
            *compute_scratch(),
        ],
        compiler_params=pltpu.CompilerParams(collective_id=0, has_side_effects=True, vmem_limit_bytes=67043328),
        name="whole_step",
    )(*args)


def split_kernel(res, loss_ref, e_out, wg_out, wu_out, wd_out):
    loss_ref[0, 0] = res[RS_LOSS, 0]
    e_out[:, 0:128] = res[0:16, :]
    e_out[:, 128:256] = res[16:32, :]
    for base, ref in ((RS_GATE, wg_out), (RS_UP, wu_out), (RS_DOWN, wd_out)):
        tiles = ref.shape[1] // 128
        for r in range(ref.shape[0]):
            for c in range(tiles):
                row = base + r * tiles + c
                ref[r:r + 1, c * 128:(c + 1) * 128] = res[row:row + 1, :]


def split_result(res):
    vm = pl.BlockSpec(memory_space=pltpu.VMEM)
    sds = lambda *shape: jax.ShapeDtypeStruct(shape, jnp.float32)
    return pl.pallas_call(
        split_kernel,
        out_shape=(sds(1, 1), sds(16, 256), sds(2, 768), sds(2, 768), sds(6, 256)),
        in_specs=[vm],
        out_specs=(pl.BlockSpec(memory_space=pltpu.SMEM), vm, vm, vm, vm),
        compiler_params=pltpu.CompilerParams(vmem_limit_bytes=1 << 20),
        name="split_result",
    )(res)


def solution(mesh):
    def device_step(tok_ids, tok_labels, loss_mask, table_shard, gain_mlp, gain_head, gate_shard, up_shard, down_shard):
        tok = lambda t: t.reshape(N_TILE, 1, TILE)
        loss, e_out, wg_out, wu_out, wd_out = split_result(whole_step(table_shard, gate_shard, up_shard, down_shard, tok(tok_ids), tok(tok_labels), tok(loss_mask), gain_mlp.reshape(1, 256), gain_head.reshape(1, 256)))
        return loss[0, 0], e_out, wg_out, wu_out, wd_out

    row_spec = P("fsdp", None)
    tok_spec = P("fsdp")
    return jax.shard_map(device_step, mesh=mesh, in_specs=(tok_spec, tok_spec, tok_spec, row_spec, P(), P(), row_spec, row_spec, row_spec), out_specs=(P(), row_spec, row_spec, row_spec, row_spec), check_vma=False)
```

```python
import functools

import jax
import jax.numpy as jnp
from jax import lax
from jax.experimental import pallas as pl
from jax.experimental.pallas import tpu as pltpu
from jax.sharding import PartitionSpec as P

NORM_EPS = 1e-6
ROW_CONTRACT = (((1,), (1,)), ((), ()))
MESH = pl.DeviceIdType.MESH
AXIS = "fsdp"
STRIDES = (2, 8, 32)
N_STREAM = 6
AG_ROWS = 96
RS_ROWS = 72
RS_GATE, RS_UP, RS_DOWN, RS_LOSS = 32, 44, 56, 68
RS_STREAMS = tuple((8 * j, 8, j % 6) for j in range(9))
RS_TABLE, RS_WEIGHTS = (0, 1, 2, 3), (4, 5, 6, 7, 8)
N_RS = len(RS_STREAMS)


TILE = 1024
N_TILE = 4096 // TILE
V_CHUNK = 256
F_CHUNK = 384
TG_CHUNK = 1024


LANES, VOCAB, D_MODEL, D_FF = 128, 2048, 256, 768


def torus_partner(v, t):
    near = v + 1 - 2 * lax.rem(v, 2)
    far = 3 - v
    return near + t * (far - near)


def my_place():
    me = lax.axis_index(AXIS)
    core = lax.rem(me, 2)
    coords = (lax.rem(lax.div(me, 2), 4), lax.rem(lax.div(me, 8), 4), lax.div(me, 32))
    return me, core, coords


def greet(me, core, coords):
    barrier = pltpu.get_barrier_semaphore()
    pl.semaphore_signal(barrier, inc=1, device_id=(me + 1 - 2 * core,), device_id_type=MESH)
    for d in range(3):
        for t in range(2):
            other = me + (torus_partner(coords[d], t) - coords[d]) * STRIDES[d]
            pl.semaphore_signal(barrier, inc=1, device_id=(other,), device_id_type=MESH)
        other = me + (lax.rem(coords[d] + 2, 4) - coords[d]) * STRIDES[d]
        pl.semaphore_signal(barrier, inc=1, device_id=(other,), device_id_type=MESH)
    return barrier


def link_of(k, s, core):
    return (k + s) % 3, lax.rem(core + ((k + s) // 3) % 2, 2)


def send_copy(src, dst, send_sem, recv_sem, target):
    return pltpu.make_async_remote_copy(src_ref=src, dst_ref=dst, send_sem=send_sem, recv_sem=recv_sem, device_id=(target,), device_id_type=MESH)


def torus_order(v, t):
    return v + t * (min_int(v, 1) * (lax.rem(v, 3) + 1) - v)


def min_int(a, b):
    return jnp.minimum(a, b)


def first_pairing(k, d, core):
    return 0 if d == k % 3 else lax.rem(core + k // 3, 2)


def gather_link(k, s, core):
    t = first_pairing(k, (k + 1) % 3, core)
    return (k + 1 + s % 2) % 3, t if s < 2 else 1 - t


def gather_direct(buf, k, me, core, coords, send_sem, recv_sem):
    d = k % 3
    ref = buf.at[(core, k, *(pl.ds(torus_order(coords[e], first_pairing(k, e, core)), 1) for e in (2, 1, 0)))]
    targets = [me + (lax.rem(coords[d] + m, 4) - coords[d]) * STRIDES[d] for m in (1, 2, 3)]
    return [send_copy(ref, ref, send_sem.at[k, i], recv_sem.at[k, i], target) for i, target in enumerate(targets)]


def gather_send(buf, k, s, me, core, coords, send_sem, recv_sem):
    idx = []
    for d in (2, 1, 0):
        if d == k % 3:
            idx.append(pl.ds(0, 4))
            continue
        done = len([q for q in range(s) if (k + 1 + q % 2) % 3 == d])
        p = torus_order(coords[d], first_pairing(k, d, core))
        idx.append((pl.ds(p, 1), pl.ds(2 * lax.div(p, 2), 2), pl.ds(0, 4))[done])
    d, t = gather_link(k, s, core)
    target = me + (torus_partner(coords[d], t) - coords[d]) * STRIDES[d]
    ref = buf.at[(core, k, *idx)]
    return send_copy(ref, ref, send_sem.at[k, 3 + s], recv_sem.at[k, 3 + s], target)


def side_send_half(buf, k, late, me, core, coords, side_send, side_recv):
    d, _ = gather_link(k, 3, core)
    p = lax.div(torus_order(coords[d], first_pairing(k, d, core)), 2)
    idx = [pl.ds(0, 4)] * 3
    idx[2 - d] = pl.ds(2 * (p + late * (1 - 2 * p)), 2)
    ref = buf.at[(core, k, *idx)]
    return send_copy(ref, ref, side_send.at[k, late], side_recv.at[k, late], me + 1 - 2 * core)


def gather_phase(me, core, coords, barrier, early, shards, mask, buf, pack, send_sem, recv_sem, side_send, side_recv):
    cx, cy, cz = coords
    wide = jnp.float32
    e_ref, *w_refs = shards
    pack[0:16, :] = e_ref[:, 0:LANES].astype(wide)
    pack[16:32, :] = e_ref[:, LANES:D_MODEL].astype(wide)
    pack[32:AG_ROWS, :] = jnp.zeros((AG_ROWS - 32, LANES), wide)
    for k, ref in enumerate(w_refs):
        vals = ref[...].astype(wide)
        tiles = vals.shape[1] // LANES
        for r in range(vals.shape[0]):
            for c in range(tiles):
                row = 32 + 16 * k + r * tiles + c
                pack[row:row + 1, :] = vals[r:r + 1, c * LANES:(c + 1) * LANES]
    counts = jnp.zeros((1, LANES), wide)
    for i in range(N_TILE):
        row = mask[i].astype(wide)
        for c in range(TILE // LANES):
            counts += row[:, c * LANES:(c + 1) * LANES]
    pack[80:81, :] = counts
    for k in range(N_STREAM):
        pz, py, px = (torus_order(coords[d], first_pairing(k, d, core)) for d in (2, 1, 0))
        buf[core, k, pz, py, px] = pack[16 * k:16 * k + 16, :].astype(jnp.bfloat16)
    pl.semaphore_wait(barrier, 10)
    sent = []
    flight = []
    sides = []
    for k in range(N_STREAM):
        flight.append(gather_direct(buf, k, me, core, coords, send_sem, recv_sem))
        for c in flight[k]:
            c.start()
    early()
    for s in range(4):
        for k in range(N_STREAM):
            for c in flight[k]:
                c.wait_recv()
            sent += flight[k]
            flight[k] = [gather_send(buf, k, s, me, core, coords, send_sem, recv_sem)]
            flight[k][0].start()
            if s == 3:
                sides.append(side_send_half(buf, k, 0, me, core, coords, side_send, side_recv))
                sides[-1].start()
                sent += flight[k]
    return sent, flight, sides


def gathered_blocks(k):
    order = ((0, 1, 2, 3), (0, 2, 3, 1))
    for core in range(2):
        first = [0 if d == k % 3 else (core + k // 3) % 2 for d in range(3)]
        for z in range(4):
            for y in range(4):
                for x in range(4):
                    yield ((z * 4 + y) * 4 + x) * 2 + core, (core, k, order[first[2]][z], order[first[1]][y], order[first[0]][x])


def recv_shape(k, s):
    sizes = [4, 4, 4]
    for q in range(s + 1):
        sizes[(k + q) % 3] //= 2
    return sizes[2], sizes[1], sizes[0]


class Reducer:
    def __init__(self, me, core, coords, g, side, res, recv, send_sem, recv_sem, side_send, side_recv):
        self.me, self.core, self.coords = me, core, coords
        self.g, self.side, self.res, self.recv = g, side, res, recv
        self.sems = (send_sem, recv_sem, side_send, side_recv)
        self.flight = [None] * N_RS
        self.stage = [0] * N_RS
        self.stay = [None] * N_RS
        self.sent = []

    def at_dim(self, d, idx):
        full = [slice(None)] * 3
        full[2 - d] = idx
        return tuple(full)

    def halves(self, j, core):
        d, t = link_of(RS_STREAMS[j][2], 0, core)
        v = self.coords[d]
        mate = torus_partner(v, t)
        far, near = torus_partner(mate, 1 - t), torus_partner(v, 1 - t)
        return (jnp.minimum(mate, far), jnp.maximum(mate, far)), (jnp.minimum(v, near), jnp.maximum(v, near))

    def cross(self, j, i, idx):
        r0, rn, k = RS_STREAMS[j]
        z, y, x = self.at_dim(k % 3, pl.ds(idx, 1))
        rows = pl.ds(r0, rn)
        return send_copy(self.g.at[z, y, x, 1 - self.core, rows, :], self.side.at[z, y, x, rows, :], self.sems[2].at[j, i], self.sems[3].at[j, i], self.me + 1 - 2 * self.core)

    def start_stay(self):
        for copies in self.stay:
            for c in copies:
                c.start()
            self.sent += copies

    def post(self, j, copies):
        for c in copies:
            c.start()
        self.flight[j] = copies
        self.sent += copies

    def advance(self, j):
        me, core, coords = self.me, self.core, self.coords
        send_sem, recv_sem, side_send, side_recv = self.sems
        r0, rn, k = RS_STREAMS[j]
        rows = pl.ds(r0, rn)
        stage = self.stage[j]
        self.stage[j] += 1
        if stage == 0:
            leave, stay = self.halves(j, 1 - core)
            self.post(j, [self.cross(j, i, idx) for i, idx in enumerate(leave)])
            self.stay[j] = [self.cross(j, 2 + i, idx) for i, idx in enumerate(stay)]
            return
        for c in self.flight[j]:
            c.wait_recv()
        if stage == 1:
            d, _ = link_of(k, 0, core)
            for idx in self.halves(j, core)[0]:
                z, y, x = self.at_dim(d, pl.ds(idx, 1))
                self.side[z, y, x, rows, :] += self.g[z, y, x, core, rows, :]
            cur = self.side.at[:, :, :, rows, :]
        else:
            q = stage - 2
            d, t = link_of(k, q, core)
            v = coords[d]
            prev = self.side.at[:, :, :, rows, :] if q == 0 else self.recv[j * 6 + q - 1]
            cur = self.recv[j * 6 + q]
            if q < 3:
                mate = torus_partner(v, 1 - t)
                if q == 0:
                    for c in self.stay[j]:
                        c.wait_recv()
                for i, idx in enumerate((jnp.minimum(v, mate), jnp.maximum(v, mate))):
                    at = self.at_dim(d, pl.ds(idx, 1))
                    own = prev[at]
                    if q == 0:
                        own += self.g[(*at, core, rows, slice(None))]
                    cur[self.at_dim(d, pl.ds(i, 1))] += own
            else:
                mate = torus_partner(v, t)
                keep = jnp.where(v > mate, 1, 0)
                cur[...] += prev[self.at_dim(d, pl.ds(keep, 1))]
        s = stage - 1
        if s == 6:
            self.res[rows, :] = cur[0, 0, 0]
            return
        d, t = link_of(k, s, core)
        v = coords[d]
        mate = torus_partner(v, t)
        target = me + (mate - v) * STRIDES[d]
        dst = self.recv[j * 6 + s]
        if s < 3:
            far = torus_partner(mate, 1 - t)
            copies = [send_copy(cur.at[self.at_dim(d, pl.ds(idx, 1))], dst.at[self.at_dim(d, pl.ds(i, 1))], send_sem.at[j, 2 * s + i], recv_sem.at[j, 2 * s + i], target) for i, idx in enumerate((jnp.minimum(mate, far), jnp.maximum(mate, far)))]
        else:
            give = jnp.where(v > mate, 0, 1)
            copies = [send_copy(cur.at[self.at_dim(d, pl.ds(give, 1))], dst, send_sem.at[j, 3 + s], recv_sem.at[j, 3 + s], target)]
        self.post(j, copies)


def mm(a, b):
    return jnp.dot(a, b, preferred_element_type=jnp.float32)


def mm_nt(a, b):
    return lax.dot_general(a, b, ROW_CONTRACT, preferred_element_type=jnp.float32)


def compute_scratch():
    v = lambda dt, *shape: pltpu.VMEM(shape, dt)
    f32, bf16 = jnp.float32, jnp.bfloat16
    return [
        v(bf16, VOCAB, D_MODEL), v(bf16, D_MODEL, VOCAB),
        v(bf16, D_MODEL, D_FF), v(bf16, D_FF, D_MODEL), v(bf16, D_MODEL, D_FF), v(bf16, D_FF, D_MODEL), v(bf16, D_FF, D_MODEL), v(bf16, D_MODEL, D_FF),
        v(f32, D_MODEL, LANES), v(f32, D_MODEL, LANES), v(f32, 1, TILE),
        v(f32, VOCAB, D_MODEL), v(f32, D_MODEL, D_FF), v(f32, D_MODEL, D_FF), v(f32, D_FF, D_MODEL),
        v(f32, VOCAB, TILE), v(bf16, VOCAB, TILE), v(bf16, VOCAB, TILE),
        v(f32, D_FF, TILE), v(f32, D_FF, TILE), v(bf16, D_FF, TILE), v(bf16, D_FF, TILE), v(bf16, D_FF, TILE), v(f32, 1536, LANES),
        v(f32, VOCAB, D_MODEL), v(bf16, VOCAB, LANES), v(bf16, D_MODEL, VOCAB), v(f32, 8, VOCAB),
        v(f32, 1024, D_MODEL), v(f32, 8, 1024),
    ]


def early_phase(g1, g2, e_s, et_s, wg_s, wgt_s, wu_s, wut_s, wd_s, wdt_s, g1_s, g2_s, loss_s, d_e, d_wg, d_wu, d_wd, logit_s, dl_s, oh_s, sl_s, dp_s, u_s, dq_s, dpb_s, stage, s_acc, cnt_s, hn_s, n_s, s_in, n_in):
    g1_s[...] = jnp.broadcast_to(g1[...], (LANES, D_MODEL)).T
    g2_s[...] = jnp.broadcast_to(g2[...], (LANES, D_MODEL)).T
    d_e[...] = jnp.zeros_like(d_e)
    loss_s[...] = jnp.zeros_like(loss_s)
    cnt_s[...] = jnp.zeros_like(cnt_s)
    s_acc[...] = jnp.zeros_like(s_acc)


def compute_phase(buf, ids, labels, mask, g1, g2, g, reducer, ready, core, to_sibling, e_s, et_s, wg_s, wgt_s, wu_s, wut_s, wd_s, wdt_s, g1_s, g2_s, loss_s, d_e, d_wg, d_wu, d_wd, logit_s, dl_s, oh_s, sl_s, dp_s, u_s, dq_s, dpb_s, stage, s_acc, cnt_s, hn_s, n_s, s_in, n_in):
    f32, bf16 = jnp.float32, jnp.bfloat16
    for half in range(2):
        ready(half)
        for dev, place in gathered_blocks(half):
            e_s[16 * dev:16 * dev + 16, LANES * half:LANES * half + LANES] = buf[place]
        et_s[LANES * half:LANES * half + LANES, :] = e_s[:, LANES * half:LANES * half + LANES].T

    def wide_gain(ref):
        return jnp.concatenate([ref[...]] * (TILE // LANES), axis=1)

    def norm(x, gain):
        r = lax.rsqrt(jnp.mean(x * x, axis=0, keepdims=True) + NORM_EPS)
        return (x * r * gain).astype(bf16), r

    def norm_back(x, r, gain, grad):
        sg = grad * gain
        return r * (sg - x * (r * r) * jnp.mean(sg * x, axis=0, keepdims=True))

    def one_hots(i):
        id_row = jnp.where(mask[i] == 1, ids[i], -1)
        label_row = labels[i]
        for v in range(0, VOCAB, V_CHUNK):
            vocab = lax.broadcasted_iota(jnp.int32, (V_CHUNK, TILE), 0) + v
            oh_s[v:v + V_CHUNK, :] = jnp.where(vocab == id_row, 1.0, 0.0).astype(bf16)
            dl_s[v:v + V_CHUNK, :] = jnp.where(vocab == label_row, 1.0, 0.0).astype(bf16)

    def label_rows(i, carry):
        one_hots(i)
        picked = mm(et_s[...], dl_s[...]).astype(bf16)
        for v in range(0, VOCAB, TG_CHUNK):
            sl = slice(v, v + TG_CHUNK)
            s_acc[sl, :] += mm_nt(oh_s[sl, :], picked)
        for v in range(0, VOCAB, V_CHUNK):
            sl = slice(v, v + V_CHUNK)
            count = cnt_s[sl, :]
            for c in range(0, TILE, LANES):
                count += oh_s[sl, c:c + LANES]
            cnt_s[sl, :] = count
        return carry

    def hidden_rows(i):
        one_hots(i)
        picked = mm(hn_s[...], oh_s[...]).astype(bf16)
        for v in range(0, VOCAB, TG_CHUNK):
            sl = slice(v, v + TG_CHUNK)
            s_acc[sl, :] += mm_nt(dl_s[sl, :], picked)

    def row_step():
        x = et_s[:, at].astype(f32)
        label_sum = s_acc[at, :].T
        n_row = n_s[0:1, at]
        gain1, gain2 = wide_gain(g1_s), wide_gain(g2_s)
        a, r1 = norm(x, gain1)
        for f in range(0, D_FF, F_CHUNK):
            sl = slice(f, f + F_CHUNK)
            p = mm(wgt_s[sl, :], a).astype(bf16).astype(f32)
            q = mm(wut_s[sl, :], a).astype(bf16).astype(f32)
            s = jax.nn.sigmoid(p)
            silu = p * s
            sl_s[sl, :] = silu
            u_s[sl, :] = (silu * q).astype(bf16)
            dp_s[sl, :] = q * (s + silu * (1.0 - s))
        h = (x + mm(wdt_s[...], u_s[...])).astype(bf16).astype(f32)
        hn, r2 = norm(h, gain2)
        hn_s[:, at] = hn
        hidden.start()
        top = jnp.full((1, TILE), -jnp.inf, f32)
        for v in range(0, VOCAB, V_CHUNK):
            part = mm(e_s[v:v + V_CHUNK, :], hn)
            logit_s[v:v + V_CHUNK, :] = part
            top = jnp.maximum(top, jnp.max(part, axis=0, keepdims=True))
        den = jnp.zeros((1, TILE), f32)
        for v in range(0, VOCAB, V_CHUNK):
            part = jnp.exp(logit_s[v:v + V_CHUNK, :] - top)
            den += jnp.sum(part, axis=0, keepdims=True)
            logit_s[v:v + V_CHUNK, :] = part
        picked = jnp.sum(hn.astype(f32) * label_sum, axis=0, keepdims=True)
        loss_s[...] += coef * (n_row * (top + jnp.log(den)) - picked)
        scale = coef * n_row / den
        for v in range(0, VOCAB, V_CHUNK):
            dl_s[v:v + V_CHUNK, :] = (logit_s[v:v + V_CHUNK, :] * scale).astype(bf16)
        dhn = mm(et_s[...], dl_s[...]) - coef * label_sum
        dh = norm_back(h, r2, gain2, dhn)
        dhb = dh.astype(bf16)
        for f in range(0, D_FF, F_CHUNK):
            sl = slice(f, f + F_CHUNK)
            du = mm(wd_s[sl, :], dhb)
            dq_s[sl, :] = (du * sl_s[sl, :]).astype(bf16)
            dpb_s[sl, :] = (du * dp_s[sl, :]).astype(bf16)
            d_wd[sl, :] += mm_nt(u_s[sl, :], dhb)
        d_wg[...] += mm_nt(a, dpb_s[...])
        d_wu[...] += mm_nt(a, dq_s[...])
        da = mm(wg_s[...], dpb_s[...]) + mm(wu_s[...], dq_s[...])
        dx = dh + norm_back(x, r1, gain1, da)
        for v in range(0, VOCAB, TG_CHUNK):
            sl = slice(v, v + TG_CHUNK)
            d_e[sl, :] += mm_nt(dl_s[sl, :], hn)
        d_e[at, :] += dx.T

    lax.fori_loop(0, N_TILE, label_rows, 0)
    n_s[...] = mm_nt(jnp.ones((8, LANES), bf16), cnt_s[...])
    at = pl.ds(pl.multiple_of(core * 1024, 1024), 1024)
    away = pl.ds(pl.multiple_of((1 - core) * 1024, 1024), 1024)
    sums = [to_sibling(0, s_acc.at[away, :], s_in), to_sibling(1, n_s.at[:, away], n_in)]
    for c in sums:
        c.start()
    rows = g.reshape(LANES * RS_ROWS, LANES)
    for j in range(3):
        ready(2 + j)
        for dev, place in gathered_blocks(2 + j):
            rows[dev * RS_ROWS + 16 * j:dev * RS_ROWS + 16 * j + 16, :] = buf[place].astype(f32)
    ready(5)
    total = jnp.sum(buf[:, 5, :, :, :, 0:16, :].astype(f32))
    for j, (acc, w, wt) in enumerate(((d_wg, wg_s, wgt_s), (d_wu, wu_s, wut_s), (d_wd, wd_s, wdt_s))):
        n = acc.shape[0]
        per, tiles = n // LANES, acc.shape[1] // LANES
        for c in range(tiles):
            for r in range(per):
                stage[pl.ds(c * n + r, LANES, stride=per), :] = rows[pl.ds(16 * j + r * tiles + c, LANES, stride=RS_ROWS), :]
            acc[:, c * LANES:(c + 1) * LANES] = stage[c * n:(c + 1) * n, :]
        w[...] = acc[...].astype(bf16)
        wt[...] = acc[...].T.astype(bf16)
        acc[...] = jnp.zeros_like(acc)
    coef = 1.0 / total
    for c in sums:
        c.wait_recv()
    s_acc[at, :] += s_in[...]
    n_s[:, at] += n_in[...]
    hidden = to_sibling(2, hn_s.at[:, at], hn_s.at[:, at])
    row_step()

    for base, acc in ((RS_GATE, d_wg), (RS_UP, d_wu), (RS_DOWN, d_wd)):
        n = acc.shape[0]
        per, tiles = n // LANES, acc.shape[1] // LANES
        for c in range(tiles):
            stage[c * n:(c + 1) * n, :] = acc[:, c * LANES:(c + 1) * LANES]
            for r in range(per):
                rows[pl.ds(base + r * tiles + c, LANES, stride=RS_ROWS), :] = stage[pl.ds(c * n + r, LANES, stride=per), :]
    loss = jnp.sum(loss_s[...])
    for r in range(RS_LOSS, RS_ROWS):
        rows[pl.ds(r, LANES, stride=RS_ROWS), :] = jnp.full((LANES, LANES), loss, f32)
    for c in sums:
        c.wait_send()
    s_acc[...] = jnp.zeros_like(s_acc)
    hidden.wait()
    lax.fori_loop(0, N_TILE, lambda i, c: (hidden_rows(i), c)[1], 0)
    for half in range(2):
        cols = slice(LANES * half, LANES * half + LANES)
        g[:, :, :, :, 16 * half:16 * half + 16, :] = (d_e[:, cols] - coef * s_acc[:, cols]).reshape(4, 4, 4, 2, 16, LANES)
    for j in RS_TABLE + RS_WEIGHTS:
        reducer.advance(j)
    reducer.start_stay()
    while min(reducer.stage) < 8:
        for j in RS_TABLE + RS_WEIGHTS:
            if reducer.stage[j] < 8:
                reducer.advance(j)


def whole_kernel(*refs):
    me, core, coords = my_place()
    barrier = greet(me, core, coords)
    n_in = 9
    sources, res_out, local, in_sem = refs[:n_in], refs[n_in], refs[n_in + 1:2 * n_in + 1], refs[2 * n_in + 1]
    refs = refs[2 * n_in + 2:]
    buf, pack, side, g = refs[:4]
    recv = refs[4:4 + 6 * N_RS]
    ag_send, ag_recv, ag_side_send, ag_side_recv = refs[4 + 6 * N_RS:8 + 6 * N_RS]
    rs_sems = refs[8 + 6 * N_RS:12 + 6 * N_RS]
    pair_sems = refs[12 + 6 * N_RS:14 + 6 * N_RS]
    scratch = refs[14 + 6 * N_RS:]
    loads = [pltpu.make_async_copy(src, dst, in_sem.at[i]) for i, (src, dst) in enumerate(zip(sources, local))]
    for c in loads:
        c.start()
    for c in loads:
        c.wait()
    *shards, ids, labels, mask, g1, g2 = local
    sent, flight, sides = gather_phase(me, core, coords, barrier, lambda: early_phase(g1, g2, *scratch), shards, mask, buf, pack, ag_send, ag_recv, ag_side_send, ag_side_recv)
    late = []
    for k in range(N_STREAM):
        flight[k][0].wait_recv()
        late.append(side_send_half(buf, k, 1, me, core, coords, ag_side_send, ag_side_recv))
        late[k].start()

    def ready(k):
        sides[k].wait_recv()
        late[k].wait_recv()

    reducer = Reducer(me, core, coords, g, side, res_out, recv, *rs_sems)

    def to_sibling(i, src, dst):
        return send_copy(src, dst, pair_sems[0].at[i], pair_sems[1].at[i], me + 1 - 2 * core)

    compute_phase(buf, ids, labels, mask, g1, g2, g, reducer, ready, core, to_sibling, *scratch)
    for c in sent + sides + late + reducer.sent:
        c.wait_send()


def whole_step(*args):
    vm = pl.BlockSpec(memory_space=pltpu.VMEM)
    v = lambda dt, *shape: pltpu.VMEM(shape, dt)
    f32 = jnp.float32
    recvs = [v(f32, *recv_shape(k, s), rn, LANES) for _, rn, k in RS_STREAMS for s in range(6)]
    sem = pltpu.SemaphoreType.DMA
    return pl.pallas_call(
        whole_kernel,
        out_shape=jax.ShapeDtypeStruct((RS_ROWS, LANES), f32),
        in_specs=[pl.BlockSpec(memory_space=pl.ANY)] * 9,
        out_specs=vm,
        scratch_shapes=[
            *[v(a.dtype, *a.shape) for a in args],
            sem((9,)),
            v(jnp.bfloat16, 2, N_STREAM, 4, 4, 4, 16, LANES), v(f32, AG_ROWS, LANES),
            v(f32, 4, 4, 4, RS_ROWS, LANES), v(f32, 4, 4, 4, 2, RS_ROWS, LANES),
            *recvs,
            sem((N_STREAM, 7)), sem((N_STREAM, 7)), sem((N_STREAM, 2)), sem((N_STREAM, 2)),
            sem((N_RS, 9)), sem((N_RS, 9)), sem((N_RS, 4)), sem((N_RS, 4)), sem((3,)), sem((3,)),
            *compute_scratch(),
        ],
        compiler_params=pltpu.CompilerParams(collective_id=0, has_side_effects=True, vmem_limit_bytes=67043328),
        name="whole_step",
    )(*args)


def split_kernel(res, loss_ref, e_out, wg_out, wu_out, wd_out):
    loss_ref[0, 0] = res[RS_LOSS, 0]
    e_out[:, 0:LANES] = res[0:16, :]
    e_out[:, LANES:D_MODEL] = res[16:32, :]
    for base, ref in ((RS_GATE, wg_out), (RS_UP, wu_out), (RS_DOWN, wd_out)):
        tiles = ref.shape[1] // LANES
        for r in range(ref.shape[0]):
            for c in range(tiles):
                row = base + r * tiles + c
                ref[r:r + 1, c * LANES:(c + 1) * LANES] = res[row:row + 1, :]


def split_result(res):
    vm = pl.BlockSpec(memory_space=pltpu.VMEM)
    sds = lambda *shape: jax.ShapeDtypeStruct(shape, jnp.float32)
    return pl.pallas_call(
        split_kernel,
        out_shape=(sds(1, 1), sds(16, D_MODEL), sds(2, D_FF), sds(2, D_FF), sds(6, D_MODEL)),
        in_specs=[vm],
        out_specs=(pl.BlockSpec(memory_space=pltpu.SMEM), vm, vm, vm, vm),
        compiler_params=pltpu.CompilerParams(vmem_limit_bytes=1 << 20),
        name="split_result",
    )(res)


def solution(mesh):
    def device_step(tok_ids, tok_labels, loss_mask, table_shard, gain_mlp, gain_head, gate_shard, up_shard, down_shard):
        tok = lambda t: t.reshape(N_TILE, 1, TILE)
        loss, e_out, wg_out, wu_out, wd_out = split_result(whole_step(table_shard, gate_shard, up_shard, down_shard, tok(tok_ids), tok(tok_labels), tok(loss_mask), gain_mlp.reshape(1, D_MODEL), gain_head.reshape(1, D_MODEL)))
        return loss[0, 0], e_out, wg_out, wu_out, wd_out

    row_spec = P("fsdp", None)
    tok_spec = P("fsdp")
    return jax.shard_map(device_step, mesh=mesh, in_specs=(tok_spec, tok_spec, tok_spec, row_spec, P(), P(), row_spec, row_spec, row_spec), out_specs=(P(), row_spec, row_spec, row_spec, row_spec), check_vma=False)
```

```python
import functools

import jax
import jax.numpy as jnp
from jax import lax
from jax.experimental import pallas as pl
from jax.experimental.pallas import tpu as pltpu
from jax.sharding import PartitionSpec as P

NORM_EPS = 1e-6
ROW_CONTRACT = (((1,), (1,)), ((), ()))
MESH = pl.DeviceIdType.MESH
AXIS = "fsdp"
STRIDES = (2, 8, 32)
N_STREAM = 6
AG_ROWS = 96
RS_ROWS = 72
RS_GATE, RS_UP, RS_DOWN, RS_LOSS = 32, 44, 56, 68
RS_STREAMS = tuple((8 * j, 8, j % 6) for j in range(9))
RS_TABLE, RS_WEIGHTS = (0, 1, 2, 3), (4, 5, 6, 7, 8)
N_RS = len(RS_STREAMS)


TILE = 1024
N_TILE = 4096 // TILE
V_CHUNK = 256
F_CHUNK = 384
TG_CHUNK = 1024


LANES, VOCAB, D_MODEL, D_FF = 128, 2048, 256, 768


def torus_partner(v, t):
    near = v + 1 - 2 * lax.rem(v, 2)
    far = 3 - v
    return near + t * (far - near)


def my_place():
    me = lax.axis_index(AXIS)
    core = lax.rem(me, 2)
    coords = (lax.rem(lax.div(me, 2), 4), lax.rem(lax.div(me, 8), 4), lax.div(me, 32))
    return me, core, coords


def greet(me, core, coords):
    barrier = pltpu.get_barrier_semaphore()
    pl.semaphore_signal(barrier, inc=1, device_id=(me + 1 - 2 * core,), device_id_type=MESH)
    for d in range(3):
        for t in range(2):
            other = me + (torus_partner(coords[d], t) - coords[d]) * STRIDES[d]
            pl.semaphore_signal(barrier, inc=1, device_id=(other,), device_id_type=MESH)
        other = me + (lax.rem(coords[d] + 2, 4) - coords[d]) * STRIDES[d]
        pl.semaphore_signal(barrier, inc=1, device_id=(other,), device_id_type=MESH)
    return barrier


def link_of(k, s, core):
    return (k + s) % 3, lax.rem(core + ((k + s) // 3) % 2, 2)


def send_copy(src, dst, send_sem, recv_sem, target):
    return pltpu.make_async_remote_copy(src_ref=src, dst_ref=dst, send_sem=send_sem, recv_sem=recv_sem, device_id=(target,), device_id_type=MESH)


def torus_order(v, t):
    return v + t * (min_int(v, 1) * (lax.rem(v, 3) + 1) - v)


def min_int(a, b):
    return jnp.minimum(a, b)


def first_pairing(k, d, core):
    return 0 if d == k % 3 else lax.rem(core + k // 3, 2)


def gather_link(k, s, core):
    t = first_pairing(k, (k + 1) % 3, core)
    return (k + 1 + s % 2) % 3, t if s < 2 else 1 - t


def gather_direct(buf, k, me, core, coords, send_sem, recv_sem):
    d = k % 3
    ref = buf.at[(core, k, *(pl.ds(torus_order(coords[e], first_pairing(k, e, core)), 1) for e in (2, 1, 0)))]
    targets = [me + (lax.rem(coords[d] + m, 4) - coords[d]) * STRIDES[d] for m in (1, 2, 3)]
    return [send_copy(ref, ref, send_sem.at[k, i], recv_sem.at[k, i], target) for i, target in enumerate(targets)]


def gather_send(buf, k, s, me, core, coords, send_sem, recv_sem):
    idx = []
    for d in (2, 1, 0):
        if d == k % 3:
            idx.append(pl.ds(0, 4))
            continue
        done = len([q for q in range(s) if (k + 1 + q % 2) % 3 == d])
        p = torus_order(coords[d], first_pairing(k, d, core))
        idx.append((pl.ds(p, 1), pl.ds(2 * lax.div(p, 2), 2), pl.ds(0, 4))[done])
    d, t = gather_link(k, s, core)
    target = me + (torus_partner(coords[d], t) - coords[d]) * STRIDES[d]
    ref = buf.at[(core, k, *idx)]
    return send_copy(ref, ref, send_sem.at[k, 3 + s], recv_sem.at[k, 3 + s], target)


def side_send_half(buf, k, late, me, core, coords, side_send, side_recv):
    d, _ = gather_link(k, 3, core)
    p = lax.div(torus_order(coords[d], first_pairing(k, d, core)), 2)
    idx = [pl.ds(0, 4)] * 3
    idx[2 - d] = pl.ds(2 * (p + late * (1 - 2 * p)), 2)
    ref = buf.at[(core, k, *idx)]
    return send_copy(ref, ref, side_send.at[k, late], side_recv.at[k, late], me + 1 - 2 * core)


def gather_phase(me, core, coords, barrier, early, shards, mask, buf, pack, send_sem, recv_sem, side_send, side_recv):
    cx, cy, cz = coords
    wide = jnp.float32
    e_ref, *w_refs = shards
    pack[0:16, :] = e_ref[:, 0:LANES].astype(wide)
    pack[16:32, :] = e_ref[:, LANES:D_MODEL].astype(wide)
    pack[32:AG_ROWS, :] = jnp.zeros((AG_ROWS - 32, LANES), wide)
    for k, ref in enumerate(w_refs):
        vals = ref[...].astype(wide)
        tiles = vals.shape[1] // LANES
        for r in range(vals.shape[0]):
            for c in range(tiles):
                row = 32 + 16 * k + r * tiles + c
                pack[row:row + 1, :] = vals[r:r + 1, c * LANES:(c + 1) * LANES]
    counts = jnp.zeros((1, LANES), wide)
    for i in range(N_TILE):
        row = mask[i].astype(wide)
        for c in range(TILE // LANES):
            counts += row[:, c * LANES:(c + 1) * LANES]
    pack[80:81, :] = counts
    for k in range(N_STREAM):
        pz, py, px = (torus_order(coords[d], first_pairing(k, d, core)) for d in (2, 1, 0))
        buf[core, k, pz, py, px] = pack[16 * k:16 * k + 16, :].astype(jnp.bfloat16)
    pl.semaphore_wait(barrier, 10)
    sent = []
    flight = []
    sides = []
    for k in range(N_STREAM):
        flight.append(gather_direct(buf, k, me, core, coords, send_sem, recv_sem))
        for c in flight[k]:
            c.start()
    early()
    for s in range(4):
        for k in range(N_STREAM):
            for c in flight[k]:
                c.wait_recv()
            sent += flight[k]
            flight[k] = [gather_send(buf, k, s, me, core, coords, send_sem, recv_sem)]
            flight[k][0].start()
            if s == 3:
                sides.append(side_send_half(buf, k, 0, me, core, coords, side_send, side_recv))
                sides[-1].start()
                sent += flight[k]
    return sent, flight, sides


def gathered_blocks(k):
    order = ((0, 1, 2, 3), (0, 2, 3, 1))
    for core in range(2):
        first = [0 if d == k % 3 else (core + k // 3) % 2 for d in range(3)]
        for z in range(4):
            for y in range(4):
                for x in range(4):
                    yield ((z * 4 + y) * 4 + x) * 2 + core, (core, k, order[first[2]][z], order[first[1]][y], order[first[0]][x])


def recv_shape(k, s):
    sizes = [4, 4, 4]
    for q in range(s + 1):
        sizes[(k + q) % 3] //= 2
    return sizes[2], sizes[1], sizes[0]


class Reducer:
    def __init__(self, me, core, coords, g, side, res, recv, send_sem, recv_sem, side_send, side_recv):
        self.me, self.core, self.coords = me, core, coords
        self.g, self.side, self.res, self.recv = g, side, res, recv
        self.sems = (send_sem, recv_sem, side_send, side_recv)
        self.flight = [None] * N_RS
        self.stage = [0] * N_RS
        self.stay = [None] * N_RS
        self.sent = []

    def at_dim(self, d, idx):
        full = [slice(None)] * 3
        full[2 - d] = idx
        return tuple(full)

    def halves(self, j, core):
        d, t = link_of(RS_STREAMS[j][2], 0, core)
        v = self.coords[d]
        mate = torus_partner(v, t)
        far, near = torus_partner(mate, 1 - t), torus_partner(v, 1 - t)
        return (jnp.minimum(mate, far), jnp.maximum(mate, far)), (jnp.minimum(v, near), jnp.maximum(v, near))

    def cross(self, j, i, idx):
        r0, rn, k = RS_STREAMS[j]
        z, y, x = self.at_dim(k % 3, pl.ds(idx, 1))
        rows = pl.ds(r0, rn)
        return send_copy(self.g.at[z, y, x, 1 - self.core, rows, :], self.side.at[z, y, x, rows, :], self.sems[2].at[j, i], self.sems[3].at[j, i], self.me + 1 - 2 * self.core)

    def start_stay(self):
        for copies in self.stay:
            for c in copies:
                c.start()
            self.sent += copies

    def post(self, j, copies):
        for c in copies:
            c.start()
        self.flight[j] = copies
        self.sent += copies

    def advance(self, j):
        me, core, coords = self.me, self.core, self.coords
        send_sem, recv_sem, side_send, side_recv = self.sems
        r0, rn, k = RS_STREAMS[j]
        rows = pl.ds(r0, rn)
        stage = self.stage[j]
        self.stage[j] += 1
        if stage == 0:
            leave, stay = self.halves(j, 1 - core)
            self.post(j, [self.cross(j, i, idx) for i, idx in enumerate(leave)])
            self.stay[j] = [self.cross(j, 2 + i, idx) for i, idx in enumerate(stay)]
            return
        for c in self.flight[j]:
            c.wait_recv()
        if stage == 1:
            d, _ = link_of(k, 0, core)
            for idx in self.halves(j, core)[0]:
                z, y, x = self.at_dim(d, pl.ds(idx, 1))
                self.side[z, y, x, rows, :] += self.g[z, y, x, core, rows, :]
            cur = self.side.at[:, :, :, rows, :]
        else:
            q = stage - 2
            d, t = link_of(k, q, core)
            v = coords[d]
            prev = self.side.at[:, :, :, rows, :] if q == 0 else self.recv[j * 6 + q - 1]
            cur = self.recv[j * 6 + q]
            if q < 3:
                mate = torus_partner(v, 1 - t)
                if q == 0:
                    for c in self.stay[j]:
                        c.wait_recv()
                for i, idx in enumerate((jnp.minimum(v, mate), jnp.maximum(v, mate))):
                    at = self.at_dim(d, pl.ds(idx, 1))
                    own = prev[at]
                    if q == 0:
                        own += self.g[(*at, core, rows, slice(None))]
                    cur[self.at_dim(d, pl.ds(i, 1))] += own
            else:
                mate = torus_partner(v, t)
                keep = jnp.where(v > mate, 1, 0)
                cur[...] += prev[self.at_dim(d, pl.ds(keep, 1))]
        s = stage - 1
        if s == 6:
            self.res[rows, :] = cur[0, 0, 0]
            return
        d, t = link_of(k, s, core)
        v = coords[d]
        mate = torus_partner(v, t)
        target = me + (mate - v) * STRIDES[d]
        dst = self.recv[j * 6 + s]
        if s < 3:
            far = torus_partner(mate, 1 - t)
            copies = [send_copy(cur.at[self.at_dim(d, pl.ds(idx, 1))], dst.at[self.at_dim(d, pl.ds(i, 1))], send_sem.at[j, 2 * s + i], recv_sem.at[j, 2 * s + i], target) for i, idx in enumerate((jnp.minimum(mate, far), jnp.maximum(mate, far)))]
        else:
            give = jnp.where(v > mate, 0, 1)
            copies = [send_copy(cur.at[self.at_dim(d, pl.ds(give, 1))], dst, send_sem.at[j, 3 + s], recv_sem.at[j, 3 + s], target)]
        self.post(j, copies)


def mm(a, b):
    return jnp.dot(a, b, preferred_element_type=jnp.float32)


def mm_nt(a, b):
    return lax.dot_general(a, b, ROW_CONTRACT, preferred_element_type=jnp.float32)


def compute_scratch():
    v = lambda dt, *shape: pltpu.VMEM(shape, dt)
    f32, bf16 = jnp.float32, jnp.bfloat16
    return [
        v(bf16, VOCAB, D_MODEL), v(bf16, D_MODEL, VOCAB),
        v(bf16, D_MODEL, D_FF), v(bf16, D_FF, D_MODEL), v(bf16, D_MODEL, D_FF), v(bf16, D_FF, D_MODEL), v(bf16, D_FF, D_MODEL), v(bf16, D_MODEL, D_FF),
        v(f32, D_MODEL, LANES), v(f32, D_MODEL, LANES), v(f32, 1, TILE),
        v(f32, VOCAB, D_MODEL), v(f32, D_MODEL, D_FF), v(f32, D_MODEL, D_FF), v(f32, D_FF, D_MODEL),
        v(f32, VOCAB, TILE), v(bf16, VOCAB, TILE), v(bf16, VOCAB, TILE),
        v(f32, D_FF, TILE), v(f32, D_FF, TILE), v(bf16, D_FF, TILE), v(bf16, D_FF, TILE), v(bf16, D_FF, TILE), v(f32, 1536, LANES),
        v(f32, VOCAB, D_MODEL), v(bf16, VOCAB, LANES), v(bf16, D_MODEL, VOCAB), v(f32, 8, VOCAB),
        v(f32, 1024, D_MODEL), v(f32, 8, 1024),
    ]


def early_phase(g1, g2, e_s, et_s, wg_s, wgt_s, wu_s, wut_s, wd_s, wdt_s, g1_s, g2_s, loss_s, d_e, d_wg, d_wu, d_wd, logit_s, dl_s, oh_s, sl_s, dp_s, u_s, dq_s, dpb_s, stage, s_acc, cnt_s, hn_s, n_s, s_in, n_in):
    g1_s[...] = jnp.broadcast_to(g1[...], (LANES, D_MODEL)).T
    g2_s[...] = jnp.broadcast_to(g2[...], (LANES, D_MODEL)).T
    d_e[...] = jnp.zeros_like(d_e)
    loss_s[...] = jnp.zeros_like(loss_s)
    cnt_s[...] = jnp.zeros_like(cnt_s)
    s_acc[...] = jnp.zeros_like(s_acc)


def compute_phase(buf, ids, labels, mask, g1, g2, g, reducer, ready, forward, core, to_sibling, e_s, et_s, wg_s, wgt_s, wu_s, wut_s, wd_s, wdt_s, g1_s, g2_s, loss_s, d_e, d_wg, d_wu, d_wd, logit_s, dl_s, oh_s, sl_s, dp_s, u_s, dq_s, dpb_s, stage, s_acc, cnt_s, hn_s, n_s, s_in, n_in):
    f32, bf16 = jnp.float32, jnp.bfloat16
    for half in range(2):
        ready(half)
        for dev, place in gathered_blocks(half):
            e_s[16 * dev:16 * dev + 16, LANES * half:LANES * half + LANES] = buf[place]
        if half == 1:
            forward(range(2, N_STREAM))
        et_s[LANES * half:LANES * half + LANES, :] = e_s[:, LANES * half:LANES * half + LANES].T

    def wide_gain(ref):
        return jnp.concatenate([ref[...]] * (TILE // LANES), axis=1)

    def norm(x, gain):
        r = lax.rsqrt(jnp.mean(x * x, axis=0, keepdims=True) + NORM_EPS)
        return (x * r * gain).astype(bf16), r

    def norm_back(x, r, gain, grad):
        sg = grad * gain
        return r * (sg - x * (r * r) * jnp.mean(sg * x, axis=0, keepdims=True))

    def one_hots(i):
        id_row = jnp.where(mask[i] == 1, ids[i], -1)
        label_row = labels[i]
        for v in range(0, VOCAB, V_CHUNK):
            vocab = lax.broadcasted_iota(jnp.int32, (V_CHUNK, TILE), 0) + v
            oh_s[v:v + V_CHUNK, :] = jnp.where(vocab == id_row, 1.0, 0.0).astype(bf16)
            dl_s[v:v + V_CHUNK, :] = jnp.where(vocab == label_row, 1.0, 0.0).astype(bf16)

    def label_rows(i, carry):
        one_hots(i)
        picked = mm(et_s[...], dl_s[...]).astype(bf16)
        for v in range(0, VOCAB, TG_CHUNK):
            sl = slice(v, v + TG_CHUNK)
            s_acc[sl, :] += mm_nt(oh_s[sl, :], picked)
        for v in range(0, VOCAB, V_CHUNK):
            sl = slice(v, v + V_CHUNK)
            count = cnt_s[sl, :]
            for c in range(0, TILE, LANES):
                count += oh_s[sl, c:c + LANES]
            cnt_s[sl, :] = count
        return carry

    def hidden_rows(i):
        one_hots(i)
        picked = mm(hn_s[...], oh_s[...]).astype(bf16)
        for v in range(0, VOCAB, TG_CHUNK):
            sl = slice(v, v + TG_CHUNK)
            s_acc[sl, :] += mm_nt(dl_s[sl, :], picked)

    def row_step():
        x = et_s[:, at].astype(f32)
        label_sum = s_acc[at, :].T
        n_row = n_s[0:1, at]
        gain1, gain2 = wide_gain(g1_s), wide_gain(g2_s)
        a, r1 = norm(x, gain1)
        for f in range(0, D_FF, F_CHUNK):
            sl = slice(f, f + F_CHUNK)
            p = mm(wgt_s[sl, :], a).astype(bf16).astype(f32)
            q = mm(wut_s[sl, :], a).astype(bf16).astype(f32)
            s = jax.nn.sigmoid(p)
            silu = p * s
            sl_s[sl, :] = silu
            u_s[sl, :] = (silu * q).astype(bf16)
            dp_s[sl, :] = q * (s + silu * (1.0 - s))
        h = (x + mm(wdt_s[...], u_s[...])).astype(bf16).astype(f32)
        hn, r2 = norm(h, gain2)
        hn_s[:, at] = hn
        hidden.start()
        top = jnp.full((1, TILE), -jnp.inf, f32)
        for v in range(0, VOCAB, V_CHUNK):
            part = mm(e_s[v:v + V_CHUNK, :], hn)
            logit_s[v:v + V_CHUNK, :] = part
            top = jnp.maximum(top, jnp.max(part, axis=0, keepdims=True))
        den = jnp.zeros((1, TILE), f32)
        for v in range(0, VOCAB, V_CHUNK):
            part = jnp.exp(logit_s[v:v + V_CHUNK, :] - top)
            den += jnp.sum(part, axis=0, keepdims=True)
            logit_s[v:v + V_CHUNK, :] = part
        picked = jnp.sum(hn.astype(f32) * label_sum, axis=0, keepdims=True)
        loss_s[...] += coef * (n_row * (top + jnp.log(den)) - picked)
        scale = coef * n_row / den
        for v in range(0, VOCAB, V_CHUNK):
            dl_s[v:v + V_CHUNK, :] = (logit_s[v:v + V_CHUNK, :] * scale).astype(bf16)
        dhn = mm(et_s[...], dl_s[...]) - coef * label_sum
        dh = norm_back(h, r2, gain2, dhn)
        dhb = dh.astype(bf16)
        for f in range(0, D_FF, F_CHUNK):
            sl = slice(f, f + F_CHUNK)
            du = mm(wd_s[sl, :], dhb)
            dq_s[sl, :] = (du * sl_s[sl, :]).astype(bf16)
            dpb_s[sl, :] = (du * dp_s[sl, :]).astype(bf16)
            d_wd[sl, :] += mm_nt(u_s[sl, :], dhb)
        d_wg[...] += mm_nt(a, dpb_s[...])
        d_wu[...] += mm_nt(a, dq_s[...])
        da = mm(wg_s[...], dpb_s[...]) + mm(wu_s[...], dq_s[...])
        dx = dh + norm_back(x, r1, gain1, da)
        for v in range(0, VOCAB, TG_CHUNK):
            sl = slice(v, v + TG_CHUNK)
            d_e[sl, :] += mm_nt(dl_s[sl, :], hn)
        d_e[at, :] += dx.T

    lax.fori_loop(0, N_TILE, label_rows, 0)
    n_s[...] = mm_nt(jnp.ones((8, LANES), bf16), cnt_s[...])
    at = pl.ds(pl.multiple_of(core * 1024, 1024), 1024)
    away = pl.ds(pl.multiple_of((1 - core) * 1024, 1024), 1024)
    sums = [to_sibling(0, s_acc.at[away, :], s_in), to_sibling(1, n_s.at[:, away], n_in)]
    for c in sums:
        c.start()
    rows = g.reshape(LANES * RS_ROWS, LANES)
    for j in range(3):
        ready(2 + j)
        for dev, place in gathered_blocks(2 + j):
            rows[dev * RS_ROWS + 16 * j:dev * RS_ROWS + 16 * j + 16, :] = buf[place].astype(f32)
    ready(5)
    total = jnp.sum(buf[:, 5, :, :, :, 0:16, :].astype(f32))
    for j, (acc, w, wt) in enumerate(((d_wg, wg_s, wgt_s), (d_wu, wu_s, wut_s), (d_wd, wd_s, wdt_s))):
        n = acc.shape[0]
        per, tiles = n // LANES, acc.shape[1] // LANES
        for c in range(tiles):
            for r in range(per):
                stage[pl.ds(c * n + r, LANES, stride=per), :] = rows[pl.ds(16 * j + r * tiles + c, LANES, stride=RS_ROWS), :]
            acc[:, c * LANES:(c + 1) * LANES] = stage[c * n:(c + 1) * n, :]
        w[...] = acc[...].astype(bf16)
        wt[...] = acc[...].T.astype(bf16)
        acc[...] = jnp.zeros_like(acc)
    coef = 1.0 / total
    for c in sums:
        c.wait_recv()
    s_acc[at, :] += s_in[...]
    n_s[:, at] += n_in[...]
    hidden = to_sibling(2, hn_s.at[:, at], hn_s.at[:, at])
    row_step()

    for base, acc in ((RS_GATE, d_wg), (RS_UP, d_wu), (RS_DOWN, d_wd)):
        n = acc.shape[0]
        per, tiles = n // LANES, acc.shape[1] // LANES
        for c in range(tiles):
            stage[c * n:(c + 1) * n, :] = acc[:, c * LANES:(c + 1) * LANES]
            for r in range(per):
                rows[pl.ds(base + r * tiles + c, LANES, stride=RS_ROWS), :] = stage[pl.ds(c * n + r, LANES, stride=per), :]
    loss = jnp.sum(loss_s[...])
    for r in range(RS_LOSS, RS_ROWS):
        rows[pl.ds(r, LANES, stride=RS_ROWS), :] = jnp.full((LANES, LANES), loss, f32)
    for c in sums:
        c.wait_send()
    s_acc[...] = jnp.zeros_like(s_acc)
    hidden.wait()
    lax.fori_loop(0, N_TILE, lambda i, c: (hidden_rows(i), c)[1], 0)
    for half in range(2):
        cols = slice(LANES * half, LANES * half + LANES)
        g[:, :, :, :, 16 * half:16 * half + 16, :] = (d_e[:, cols] - coef * s_acc[:, cols]).reshape(4, 4, 4, 2, 16, LANES)
    for j in RS_TABLE + RS_WEIGHTS:
        reducer.advance(j)
    reducer.start_stay()
    while min(reducer.stage) < 8:
        for j in RS_TABLE + RS_WEIGHTS:
            if reducer.stage[j] < 8:
                reducer.advance(j)


def whole_kernel(*refs):
    me, core, coords = my_place()
    barrier = greet(me, core, coords)
    n_in = 9
    sources, res_out, local, in_sem = refs[:n_in], refs[n_in], refs[n_in + 1:2 * n_in + 1], refs[2 * n_in + 1]
    refs = refs[2 * n_in + 2:]
    buf, pack, side, g = refs[:4]
    recv = refs[4:4 + 6 * N_RS]
    ag_send, ag_recv, ag_side_send, ag_side_recv = refs[4 + 6 * N_RS:8 + 6 * N_RS]
    rs_sems = refs[8 + 6 * N_RS:12 + 6 * N_RS]
    pair_sems = refs[12 + 6 * N_RS:14 + 6 * N_RS]
    scratch = refs[14 + 6 * N_RS:]
    loads = [pltpu.make_async_copy(src, dst, in_sem.at[i]) for i, (src, dst) in enumerate(zip(sources, local))]
    for c in loads:
        c.start()
    for c in loads:
        c.wait()
    *shards, ids, labels, mask, g1, g2 = local
    sent, flight, sides = gather_phase(me, core, coords, barrier, lambda: early_phase(g1, g2, *scratch), shards, mask, buf, pack, ag_send, ag_recv, ag_side_send, ag_side_recv)
    late = []

    def forward(streams):
        for k in streams:
            flight[k][0].wait_recv()
            late.append(side_send_half(buf, k, 1, me, core, coords, ag_side_send, ag_side_recv))
            late[k].start()

    forward(range(2))

    def ready(k):
        sides[k].wait_recv()
        late[k].wait_recv()

    reducer = Reducer(me, core, coords, g, side, res_out, recv, *rs_sems)

    def to_sibling(i, src, dst):
        return send_copy(src, dst, pair_sems[0].at[i], pair_sems[1].at[i], me + 1 - 2 * core)

    compute_phase(buf, ids, labels, mask, g1, g2, g, reducer, ready, forward, core, to_sibling, *scratch)
    for c in sent + sides + late + reducer.sent:
        c.wait_send()


def whole_step(*args):
    vm = pl.BlockSpec(memory_space=pltpu.VMEM)
    v = lambda dt, *shape: pltpu.VMEM(shape, dt)
    f32 = jnp.float32
    recvs = [v(f32, *recv_shape(k, s), rn, LANES) for _, rn, k in RS_STREAMS for s in range(6)]
    sem = pltpu.SemaphoreType.DMA
    return pl.pallas_call(
        whole_kernel,
        out_shape=jax.ShapeDtypeStruct((RS_ROWS, LANES), f32),
        in_specs=[pl.BlockSpec(memory_space=pl.ANY)] * 9,
        out_specs=vm,
        scratch_shapes=[
            *[v(a.dtype, *a.shape) for a in args],
            sem((9,)),
            v(jnp.bfloat16, 2, N_STREAM, 4, 4, 4, 16, LANES), v(f32, AG_ROWS, LANES),
            v(f32, 4, 4, 4, RS_ROWS, LANES), v(f32, 4, 4, 4, 2, RS_ROWS, LANES),
            *recvs,
            sem((N_STREAM, 7)), sem((N_STREAM, 7)), sem((N_STREAM, 2)), sem((N_STREAM, 2)),
            sem((N_RS, 9)), sem((N_RS, 9)), sem((N_RS, 4)), sem((N_RS, 4)), sem((3,)), sem((3,)),
            *compute_scratch(),
        ],
        compiler_params=pltpu.CompilerParams(collective_id=0, has_side_effects=True, vmem_limit_bytes=67043328),
        name="whole_step",
    )(*args)


def split_kernel(res, loss_ref, e_out, wg_out, wu_out, wd_out):
    loss_ref[0, 0] = res[RS_LOSS, 0]
    e_out[:, 0:LANES] = res[0:16, :]
    e_out[:, LANES:D_MODEL] = res[16:32, :]
    for base, ref in ((RS_GATE, wg_out), (RS_UP, wu_out), (RS_DOWN, wd_out)):
        tiles = ref.shape[1] // LANES
        for r in range(ref.shape[0]):
            for c in range(tiles):
                row = base + r * tiles + c
                ref[r:r + 1, c * LANES:(c + 1) * LANES] = res[row:row + 1, :]


def split_result(res):
    vm = pl.BlockSpec(memory_space=pltpu.VMEM)
    sds = lambda *shape: jax.ShapeDtypeStruct(shape, jnp.float32)
    return pl.pallas_call(
        split_kernel,
        out_shape=(sds(1, 1), sds(16, D_MODEL), sds(2, D_FF), sds(2, D_FF), sds(6, D_MODEL)),
        in_specs=[vm],
        out_specs=(pl.BlockSpec(memory_space=pltpu.SMEM), vm, vm, vm, vm),
        compiler_params=pltpu.CompilerParams(vmem_limit_bytes=1 << 20),
        name="split_result",
    )(res)


def solution(mesh):
    def device_step(tok_ids, tok_labels, loss_mask, table_shard, gain_mlp, gain_head, gate_shard, up_shard, down_shard):
        tok = lambda t: t.reshape(N_TILE, 1, TILE)
        loss, e_out, wg_out, wu_out, wd_out = split_result(whole_step(table_shard, gate_shard, up_shard, down_shard, tok(tok_ids), tok(tok_labels), tok(loss_mask), gain_mlp.reshape(1, D_MODEL), gain_head.reshape(1, D_MODEL)))
        return loss[0, 0], e_out, wg_out, wu_out, wd_out

    row_spec = P("fsdp", None)
    tok_spec = P("fsdp")
    return jax.shard_map(device_step, mesh=mesh, in_specs=(tok_spec, tok_spec, tok_spec, row_spec, P(), P(), row_spec, row_spec, row_spec), out_specs=(P(), row_spec, row_spec, row_spec, row_spec), check_vma=False)
```
